128 devices in a mesh: wide: 32 (over x, z, core), narrow: 4 (over y).
Axes of the slice: x: 4, y: 4, z: 4, core: 2. Of those that a mesh axis runs over, the one named last changes fastest.
Arguments:
- cost: float32 [4096, 16384], P('wide', 'narrow'), may hold values from 0 to 2
- plan: float32 [4096, 16384], P('wide', 'narrow'), may hold values from 0 to 2
- row_mass: float32 [4096], P('wide'), may hold values from 4096 to 28672
- col_mass: float32 [16384], P('narrow'), may hold values from 1024 to 7168
- row_dual: float32 [4096], P('wide'), may hold values from -3 to 3
- col_dual: float32 [16384], P('narrow'), may hold values from -3 to 3
Outputs:
- plan_out: float32 [4096, 16384], P('wide', 'narrow')
- row_out: float32 [4096], P('wide')
- col_out: float32 [16384], P('narrow')
The draws below stay inside these ranges and needn't reach their ends.
All inputs are finite; a program needn't handle non-finite values.
Results may differ from the reference program's by a relative error of at most 0.0001.
Values sent between devices are 32-bit elements; how exact they have to be, the bound alone decides.
No kernel may reach another device: no remote copies, remote signals or barrier semaphores. Data moves between devices by JAX's collectives and lax.ppermute only.
A program may use at most 64 MiB of HBM per device.

```python
import math
import jax
import jax.numpy as jnp
from jax import lax

ITERS = 4
NR = 4096
NC = 16384


def block_scale(rng, extent, shards, smallest, largest):
    level, own = 1.0, jax.random.fold_in(rng, 6)
    for position, parts in shards:
        heights = jnp.exp(jax.random.uniform(jax.random.fold_in(own, position), (parts,), jnp.float32, smallest / len(shards), largest / len(shards)))
        level = level * jnp.repeat(heights, extent[position] // parts).reshape([-1 if axis == position else 1 for axis in range(len(extent))])
    return level


def bell_draw(rng, extent, width, limit, split=(), dtype=jnp.bfloat16):
    gain = block_scale(rng, extent, split, -0.22, 0.18) if split else 1.0
    entries = jax.random.normal(rng, extent, jnp.float32) * width * gain
    return jnp.minimum(jnp.maximum(entries, -limit), limit).astype(dtype)


def setup_inputs(seed: int = 0) -> dict:
    keys = jax.random.split(jax.random.key(seed), 7)
    cost = jnp.clip(2.0 * jax.random.uniform(keys[0], (NR, NC), jnp.float32) ** block_scale(keys[0], (NR, NC), ((0, 32), (1, 4)), -0.2, 0.2), 0.0, 2.0)
    plan = jnp.clip(2.0 * jax.random.uniform(keys[1], (NR, NC), jnp.float32) ** block_scale(keys[1], (NR, NC), ((0, 32), (1, 4)), -0.2, 0.2), 0.0, 2.0)
    row_mass = jnp.clip(4096.0 + 24576.0 * jax.random.uniform(keys[2], (NR,), jnp.float32) ** block_scale(keys[2], (NR,), ((0, 32),), -0.2, 0.2), 4096.0, 28672.0)
    col_mass = jnp.clip(1024.0 + 6144.0 * jax.random.uniform(keys[3], (NC,), jnp.float32) ** block_scale(keys[3], (NC,), ((0, 4),), -0.2, 0.2), 1024.0, 7168.0)
    row_dual = bell_draw(keys[4], (NR,), 0.5, 3.0, ((0, 32),), jnp.float32)
    col_dual = bell_draw(keys[5], (NC,), 0.5, 3.0, ((0, 4),), jnp.float32)
    return dict(cost=cost, plan=plan, row_mass=row_mass, col_mass=col_mass, row_dual=row_dual, col_dual=col_dual)


def reference(cost, plan, row_mass, col_mass, row_dual, col_dual):
    step_base = 0.9 / math.sqrt(NR + NC)
    weight = jnp.float32(step_base)
    for step in range(ITERS):
        primal_step = step_base / weight
        dual_step = step_base * weight
        fresh = jnp.maximum(plan - primal_step * (cost - row_dual[:, None] - col_dual[None, :]), 0.0)
        change = fresh - plan
        extrap = fresh + change
        moved = jnp.sum(change * change)
        new_row = row_dual + dual_step * (row_mass - lax.optimization_barrier(jnp.sum(extrap, axis=1)))
        new_col = col_dual + dual_step * (col_mass - lax.optimization_barrier(jnp.sum(extrap, axis=0)))
        dual_moved = jnp.sum((new_row - row_dual) ** 2) + jnp.sum((new_col - col_dual) ** 2)
        weight = jnp.sqrt(weight * jnp.sqrt((dual_moved + 1.0) / (moved + 1.0)))
        plan, row_dual, col_dual = (fresh, new_row, new_col)
    return (plan, row_dual, col_dual)
```

```python
import math

import jax
import jax.numpy as jnp
from jax import lax
from jax.sharding import Mesh
from jax.sharding import PartitionSpec as P

ITERS = 4
WIDE = ("wide_0", "wide_1", "wide_2")
CHIP_COLUMN = ("wide_2", "narrow")


def exchange(array, axes):
    return lax.all_to_all(array, axes, split_axis=0, concat_axis=0, tiled=True)


def shards(cost, plan, row_mass, col_mass, row_dual, col_dual):
    rows, cols = plan.shape
    half = cols // 2
    narrow_count = lax.axis_size("narrow")
    wide_count = lax.axis_size(WIDE)
    chips = wide_count // 2
    mine = lax.axis_index(("wide_0", "wide_1"))
    core = lax.axis_index("wide_2")
    column = lax.axis_index("narrow")
    step_base = 0.9 / math.sqrt(rows * wide_count + cols * narrow_count)
    weight = jnp.float32(step_base)
    row_share_mass = row_mass / narrow_count
    col_share_mass = col_mass / wide_count
    for step in range(ITERS):
        primal_step = step_base / weight
        dual_step = step_base * weight
        fresh = jnp.maximum(
            plan - primal_step * (cost - row_dual[:, None] - col_dual[None, :]), 0.0
        )
        change = fresh - plan
        extrap = fresh + change
        row_share = row_share_mass - jnp.sum(extrap, axis=1)
        col_share = col_share_mass - jnp.sum(extrap, axis=0)
        plan = fresh
        if step == ITERS - 1:
            copies = jnp.broadcast_to(col_share, (wide_count, 1, cols))
            col_left = jnp.sum(exchange(copies, WIDE), axis=(0, 1))
            row_left = jnp.sum(lax.all_gather(row_share, "narrow"), axis=0)
            row_dual = row_dual + dual_step * row_left
            col_dual = col_dual + dual_step * col_left
            break
        moved = jnp.broadcast_to(jnp.sum(change * change), (128,))
        tail = jnp.broadcast_to(jnp.concatenate([row_share, moved]), (2, rows + 128))
        sent = jnp.concatenate([col_share.reshape(2, half), tail], axis=1)
        sent = jnp.broadcast_to(sent[None], (chips, 2, half + rows + 128))
        got = exchange(sent.reshape(wide_count, 1, -1), WIDE)[:, 0]
        col_half = jnp.sum(got[:, :half], axis=0)
        row_half = lax.dynamic_index_in_dim(
            got[:, half : half + rows].reshape(chips, 2, rows), core, 1, False
        )
        scalars = jnp.stack([jnp.sum(col_half * col_half), jnp.sum(got[:, -1])])
        scalars = jnp.pad(scalars, (0, 126))
        sent = jnp.concatenate([col_half, row_half.reshape(-1), scalars])
        sent = jnp.broadcast_to(sent, (2 * narrow_count, 1, sent.shape[0]))
        got = exchange(sent, CHIP_COLUMN).reshape(2, narrow_count, -1)
        col_left = lax.dynamic_index_in_dim(got[:, :, :half], column, 1, False)
        row_left = jnp.sum(got[:, :, half : half + chips * rows], axis=1)
        left_square = jnp.sum(got[:, :, -128]) + jnp.sum(row_left * row_left)
        moved_all = 0.5 * jnp.sum(got[:, :, -127])
        own = lax.dynamic_index_in_dim(row_left.reshape(2, chips, rows), core, 0, False)
        row_dual = row_dual + dual_step * lax.dynamic_index_in_dim(own, mine, 0, False)
        col_dual = col_dual + dual_step * col_left.reshape(-1)
        dual_moved = dual_step * dual_step * left_square
        weight = jnp.sqrt(weight * jnp.sqrt((dual_moved + 1.0) / (moved_all + 1.0)))
    return (plan, row_dual, col_dual)


def solution(mesh):
    split = Mesh(
        mesh.devices.reshape(4, 4, 2, mesh.shape["narrow"]),
        ("wide_0", "wide_1", "wide_2", "narrow"),
    )
    placed = (P(WIDE, "narrow"), P(WIDE, "narrow"), P(WIDE), P("narrow"), P(WIDE), P("narrow"))
    return jax.shard_map(
        shards,
        mesh=split,
        in_specs=placed,
        out_specs=(P(WIDE, "narrow"), P(WIDE), P("narrow")),
        check_vma=False,
    )
```

```python
import functools
import math

import jax
import jax.numpy as jnp
from jax import lax
from jax.experimental import pallas as pl
from jax.experimental.pallas import tpu as pltpu
from jax.sharding import Mesh
from jax.sharding import PartitionSpec as P

ITERS = 4
LANES = 128
GROUP = 8
CHUNKS = 4
WIDE = ("wide_0", "wide_1", "wide_2")
CHIP_COLUMN = ("wide_2", "narrow")


def exchange(array, axes):
    return lax.all_to_all(array, axes, split_axis=0, concat_axis=0, tiled=True)


def total(block):
    return jnp.sum(jnp.sum(block, axis=0, keepdims=True), axis=1, keepdims=True)


def down(block):
    return jnp.sum(block, axis=0, keepdims=True)


def dual_update(got, weight, row_dual, col_dual, new_row, new_col, left_rows, sizes):
    narrow, base, half = sizes
    core, column = lax.axis_index("wide_2"), lax.axis_index("narrow")
    mine = lax.axis_index("wide_0") * lax.axis_size("wide_1") + lax.axis_index("wide_1")
    squares = jnp.zeros((GROUP, LANES), jnp.float32)
    for c in range(2):
        for r in range(0, half, GROUP):
            rows = got[c * narrow, half + r : half + r + GROUP, :]
            for n in range(1, narrow):
                rows = rows + got[c * narrow + n, half + r : half + r + GROUP, :]
            squares = squares + rows * rows
            left_rows[c * half + r : c * half + r + GROUP, :] = rows
    tails = got[0, 2 * half : 2 * half + GROUP, :]
    for n in range(1, 2 * narrow):
        tails = tails + got[n, 2 * half : 2 * half + GROUP, :]
    left_square = total(squares) + total(tails[0:1, :])
    moved = 0.5 * total(tails[1:2, :])
    old = weight[...]
    dual_step = base * old
    dual_moved = dual_step * dual_step * left_square
    fresh_weight = jnp.sqrt(old * jnp.sqrt((dual_moved + 1.0) / (moved + 1.0)))
    step = dual_step[0:1, :]
    new_row[...] = row_dual[...] + step * left_rows[pl.ds(core * half + mine, 1), :]
    for c in range(2):
        span = slice(c * half, (c + 1) * half)
        new_col[span, :] = col_dual[span, :] + step * got[c * narrow + column, 0:half, :]
    return base / fresh_weight, fresh_weight


def sweep(step, cost, plan, fresh_plan, row_all, col_dual, first, last, rows_so_far, moved, done):
    groups = len(rows_so_far)

    def tile(j, state):
        rows, moved = list(state[0]), state[1]
        lanes = pl.ds(pl.multiple_of(j * LANES, LANES), LANES)
        col = jnp.broadcast_to(col_dual[pl.ds(j, 1), :], (GROUP, LANES))
        cols = None
        for g in range(groups):
            span = slice(g * GROUP, (g + 1) * GROUP)
            old = plan[span, lanes]
            gap = cost[span, lanes] - row_all[span, :] - col
            fresh = jnp.maximum(old - step * gap, 0.0)
            change = fresh - old
            extrap = fresh + change
            fresh_plan[span, lanes] = fresh
            rows[g] = rows[g] + extrap
            cols = extrap if cols is None else cols + extrap
            moved = moved + change * change
        done(j, down(cols))
        return tuple(rows), moved

    return lax.fori_loop(first, last, tile, (tuple(rows_so_far), moved), unroll=2)


def spread_rows(row_dual, row_all):
    row_all[...] = jnp.transpose(jnp.broadcast_to(row_dual, (LANES, LANES)))


def gather_rows(rows):
    return down(jnp.transpose(jnp.concatenate(rows, axis=0)))


def zeros(groups):
    zero = jnp.zeros((GROUP, LANES), jnp.float32)
    return tuple(zero for _ in range(groups)), zero


def send_first(sent, col_mass, chips, half):
    def done(j, cols):
        upper = j // half
        lanes = pl.ds(pl.multiple_of((j - upper * half) * LANES, LANES), LANES)
        share = col_mass[pl.ds(j, 1), :] * (1.0 / (2 * chips)) - cols
        for p in range(chips):
            sent[2 * p + upper, :, lanes] = share

    return done


def send_tail(sent, chips, half, row_share, moved):
    for p in range(2 * chips):
        sent[p, :, half * LANES : (half + 1) * LANES] = row_share
        sent[p, :, (half + 1) * LANES : (half + 2) * LANES] = moved


def open_kernel(sizes, *refs):
    narrow, base, half, chips = sizes
    sources, targets, (sent, weight, row_all, sems) = refs[:6], refs[6:12], refs[12:]
    cost, plan, row_mass, col_mass, row_dual, col_dual = targets
    tiles = 2 * half // CHUNKS
    weight[...] = jnp.full((GROUP, LANES), base, jnp.float32)
    small = [pltpu.make_async_copy(sources[n], targets[n], sems.at[n, 0]) for n in range(2, 6)]
    for copy in small:
        copy.start()
    copies = []
    for k in range(CHUNKS):
        lanes = slice(k * tiles * LANES, (k + 1) * tiles * LANES)
        for n in range(2):
            copy = pltpu.make_async_copy(
                sources[n].at[:, lanes], targets[n].at[:, lanes], sems.at[n, k]
            )
            copy.start()
            copies.append(copy)
    for copy in small:
        copy.wait()
    spread_rows(row_dual[...], row_all)
    rows, moved = zeros(row_all.shape[0] // GROUP)
    done = send_first(sent, col_mass, chips, half)
    for k in range(CHUNKS):
        copies[2 * k].wait()
        copies[2 * k + 1].wait()
        rows, moved = sweep(
            jnp.float32(1.0), cost, plan, plan, row_all, col_dual,
            k * tiles, (k + 1) * tiles, rows, moved, done,
        )
    row_share = row_mass[...] * (1.0 / narrow) - gather_rows(rows)
    send_tail(sent, chips, half, row_share, down(moved))


def middle_kernel(
    sizes, got, weight, cost, plan, row_mass, col_mass, row_dual, col_dual,
    fresh_plan, sent, new_weight, new_row, new_col, row_all, left_rows,
):
    narrow, base, half, chips = sizes
    step, fresh_weight = dual_update(
        got, weight, row_dual, col_dual, new_row, new_col, left_rows, sizes[:3]
    )
    new_weight[...] = fresh_weight
    spread_rows(new_row[...], row_all)
    rows, moved = zeros(row_all.shape[0] // GROUP)
    done = send_first(sent, col_mass, chips, half)
    rows, moved = sweep(
        step, cost, plan, fresh_plan, row_all, new_col, 0, 2 * half, rows, moved, done
    )
    row_share = row_mass[...] * (1.0 / narrow) - gather_rows(rows)
    send_tail(sent, chips, half, row_share, down(moved))


def close_kernel(
    sizes, got, weight, cost, plan, row_mass, col_mass, row_dual, col_dual,
    plan_out, sent, row_sent, new_weight, new_row, new_col, row_all, left_rows, fresh_plan, sems,
):
    narrow, base, half, chips = sizes
    step, fresh_weight = dual_update(
        got, weight, row_dual, col_dual, new_row, new_col, left_rows, sizes[:3]
    )
    new_weight[...] = fresh_weight
    spread_rows(new_row[...], row_all)
    rows, moved = zeros(row_all.shape[0] // GROUP)

    def done(j, cols):
        share = col_mass[pl.ds(j, 1), :] * (1.0 / (2 * chips)) - cols
        for p in range(2 * chips):
            sent[p, pl.ds(j, 1), :] = share

    tiles = 2 * half // CHUNKS
    copies = []
    for k in range(CHUNKS):
        rows, moved = sweep(
            step, cost, plan, fresh_plan, row_all, new_col,
            k * tiles, (k + 1) * tiles, rows, moved, done,
        )
        lanes = slice(k * tiles * LANES, (k + 1) * tiles * LANES)
        copy = pltpu.make_async_copy(fresh_plan.at[:, lanes], plan_out.at[:, lanes], sems.at[k])
        copy.start()
        copies.append(copy)
    row_sent[...] = row_mass[...] * (1.0 / narrow) - gather_rows(rows)
    for copy in copies:
        copy.wait()


def reduce_kernel(sizes, got, sent, held):
    narrow, base, half, chips = sizes
    core = lax.axis_index("wide_2")
    cols = got[0]
    for p in range(1, 2 * chips):
        cols = cols + got[p]
    squares = jnp.zeros((1, LANES), jnp.float32)
    for r in range(half):
        col = cols[:, r * LANES : (r + 1) * LANES]
        squares = squares + col * col
        held[r : r + 1, :] = col
        held[half + r : half + r + 1, :] = got[2 * r + core, :, half * LANES : (half + 1) * LANES]
    moved = cols[:, (half + 1) * LANES : (half + 2) * LANES]
    place_of = lax.broadcasted_iota(jnp.int32, (GROUP, LANES), 0)
    held[2 * half : 2 * half + GROUP, :] = jnp.where(
        place_of == 0, squares, jnp.where(place_of == 1, moved, 0.0)
    )
    everything = held[...]
    for q in range(2 * narrow):
        sent[q] = everything


def finish_kernel(sizes, got, row_got, weight, row_dual, col_dual, row_out, col_out):
    narrow, base, half, chips = sizes
    cols = got[0]
    for p in range(1, 2 * chips):
        cols = cols + got[p]
    rows = row_got[0]
    for n in range(1, narrow):
        rows = rows + row_got[n]
    step = base * weight[0:1, :]
    col_out[...] = col_dual[...] + step * cols
    row_out[...] = row_dual[...] + step * rows


VM = pl.BlockSpec(memory_space=pltpu.VMEM)
HB = pl.BlockSpec(memory_space=pltpu.HBM)
ROOM = pltpu.CompilerParams(vmem_limit_bytes=16 << 20)


def shards(cost, plan, row_mass, col_mass, row_dual, col_dual):
    rows, cols = plan.shape
    tiles = cols // LANES
    half = tiles // 2
    narrow = lax.axis_size("narrow")
    wide = lax.axis_size(WIDE)
    chips = wide // 2
    base = 0.9 / math.sqrt(rows * wide + cols * narrow)
    sizes = (narrow, base, half, chips)
    row_mass, row_dual = row_mass.reshape(1, rows), row_dual.reshape(1, rows)
    col_mass, col_dual = col_mass.reshape(tiles, LANES), col_dual.reshape(tiles, LANES)

    def vm(*shape):
        return pltpu.VMEM(shape, jnp.float32)

    def near(array):
        return pltpu.with_memory_space_constraint(array, pltpu.VMEM)

    f32 = vm

    first = f32(wide, 1, (half + 2) * LANES)
    second = f32(2 * narrow, 2 * half + GROUP, LANES)
    big, state, one, many = (rows, cols), f32(GROUP, LANES), f32(1, rows), f32(tiles, LANES)
    scratch = [vm(rows, LANES), vm(2 * half, LANES)]

    inputs = (cost, plan, row_mass, col_mass, row_dual, col_dual)
    *held, sent, weight = pl.pallas_call(
        functools.partial(open_kernel, sizes),
        out_shape=(vm(*big), vm(*big), one, many, one, many, first, state),
        in_specs=[HB] * 6,
        out_specs=(VM,) * 8,
        scratch_shapes=[scratch[0], pltpu.SemaphoreType.DMA((6, CHUNKS))],
        compiler_params=ROOM,
        name="open_step",
    )(*(pltpu.with_memory_space_constraint(array, pltpu.HBM) for array in inputs))
    cost, plan, row_mass, col_mass, row_dual, col_dual = held
    for step in range(1, ITERS):
        got = exchange(sent, WIDE)
        sent = pl.pallas_call(
            functools.partial(reduce_kernel, sizes),
            out_shape=second,
            compiler_params=ROOM,
            in_specs=[VM],
            out_specs=VM,
            scratch_shapes=[vm(2 * half + GROUP, LANES)],
            name="reduce_step",
        )(near(got))
        got = exchange(sent, CHIP_COLUMN)
        operands = tuple(map(near, (got, weight, cost, plan, row_mass, col_mass, row_dual, col_dual)))
        if step < ITERS - 1:
            plan, sent, weight, row_dual, col_dual = pl.pallas_call(
                functools.partial(middle_kernel, sizes),
                out_shape=(f32(*big), first, state, one, many),
                in_specs=[VM] * 8,
                out_specs=(VM,) * 5,
                scratch_shapes=scratch,
                name="middle_step",
                compiler_params=ROOM,
            )(*operands)
        else:
            plan, sent, row_sent, weight, row_dual, col_dual = pl.pallas_call(
                functools.partial(close_kernel, sizes),
                out_shape=(jax.ShapeDtypeStruct(big, jnp.float32), vm(wide, tiles, LANES), one, state, one, many),
                in_specs=[VM] * 8,
                out_specs=(HB,) + (VM,) * 5,
                scratch_shapes=scratch + [vm(*big), pltpu.SemaphoreType.DMA((CHUNKS,))],
                name="close_step",
                compiler_params=ROOM,
            )(*operands)
    got = exchange(sent, WIDE)
    row_got = lax.all_gather(row_sent, "narrow")
    row_dual, col_dual = pl.pallas_call(
        functools.partial(finish_kernel, sizes),
        out_shape=tuple(jax.ShapeDtypeStruct(s.shape, s.dtype) for s in (one, many)),
        in_specs=[VM] * 5,
        out_specs=(VM, VM),
        name="finish_step",
        compiler_params=ROOM,
    )(near(got), row_got, weight, row_dual, col_dual)
    return (plan, row_dual.reshape(rows), col_dual.reshape(cols))


def solution(mesh):
    split = Mesh(
        mesh.devices.reshape(4, 4, 2, mesh.shape["narrow"]),
        ("wide_0", "wide_1", "wide_2", "narrow"),
    )
    placed = (P(WIDE, "narrow"), P(WIDE, "narrow"), P(WIDE), P("narrow"), P(WIDE), P("narrow"))
    return jax.shard_map(
        shards,
        mesh=split,
        in_specs=placed,
        out_specs=(P(WIDE, "narrow"), P(WIDE), P("narrow")),
        check_vma=False,
    )
```

```python
import functools
import math

import jax
import jax.numpy as jnp
from jax import lax
from jax.experimental import pallas as pl
from jax.experimental.pallas import tpu as pltpu
from jax.sharding import Mesh
from jax.sharding import PartitionSpec as P

ITERS = 4
LANES = 128
GROUP = 8
CHUNKS = 4
CORE = "wide_2"
WIDE = ("wide_0", "wide_1", "wide_2")
CHIPS = ("wide_0", "wide_1", "narrow")


def exchange(array, axes):
    return lax.all_to_all(array, axes, split_axis=0, concat_axis=0, tiled=True)


def swap(array):
    return lax.ppermute(array, CORE, [(0, 1), (1, 0)])


def total(block):
    return jnp.sum(jnp.sum(block, axis=0, keepdims=True), axis=1, keepdims=True)


def down(block):
    return jnp.sum(block, axis=0, keepdims=True)


def span(start, size):
    return pl.ds(pl.multiple_of(start * LANES, LANES), size * LANES)


def tile_of(n, size=1):
    return slice(n * LANES, (n + size) * LANES)


def dual_update(mine, theirs, own_row, weight, row_dual, col_dual, new_weight, new_row, new_col, sizes):
    base, half = sizes[1], sizes[2]
    core = lax.axis_index(CORE)
    left_square = total(mine[:, tile_of(half)]) + total(theirs[:, tile_of(half)])
    moved = total(mine[:, tile_of(half + 1)]) + total(theirs[:, tile_of(half + 1)])
    old = weight[...]
    dual_step = base * old
    dual_moved = dual_step * dual_step * left_square
    fresh_weight = jnp.sqrt(old * jnp.sqrt((dual_moved + 1.0) / (moved + 1.0)))
    new_weight[...] = fresh_weight
    new_row[...] = row_dual[...] + dual_step[0:1, :] * own_row[...]
    scale = jnp.broadcast_to(dual_step[0:1, 0:1], (1, half * LANES))
    for side, part in ((core, mine), (1 - core, theirs)):
        lanes = span(side * half, half)
        new_col[:, lanes] = col_dual[:, lanes] + scale * part[:, tile_of(0, half)]
    return base / fresh_weight


def sweep(step, cost, plan, fresh_plan, row_all, col_dual, tiles, state, done):
    first, count = tiles
    groups = len(state[0])

    def tile(n, state):
        rows, moved = list(state[0]), state[1]
        j = first + n
        lanes = span(j, 1)
        col = jnp.broadcast_to(col_dual[:, lanes], (GROUP, LANES))
        cols = None
        for g in range(groups):
            part = slice(g * GROUP, (g + 1) * GROUP)
            old = plan[part, lanes]
            gap = cost[part, lanes] - row_all[part, :] - col
            fresh = jnp.maximum(old - step * gap, 0.0)
            change = fresh - old
            extrap = fresh + change
            fresh_plan[part, lanes] = fresh
            rows[g] = rows[g] + extrap
            cols = extrap if cols is None else cols + extrap
            moved = moved + change * change
        done(n, j, down(cols))
        return tuple(rows), moved

    return lax.fori_loop(0, count, tile, state, unroll=2)


def spread_rows(row_dual, row_all):
    row_all[...] = jnp.transpose(jnp.broadcast_to(row_dual, (LANES, LANES)))


def gather_rows(rows):
    return down(jnp.transpose(jnp.concatenate(rows, axis=0)))


def zeros(row_all):
    zero = jnp.zeros((GROUP, LANES), jnp.float32)
    return tuple(zero for _ in range(row_all.shape[0] // GROUP)), zero


def into(target, col_mass, wide):
    def done(n, j, cols):
        target[:, span(n, 1)] = col_mass[:, span(j, 1)] * (1.0 / wide) - cols

    return done


def tail(keep, row_mass, state, sizes):
    narrow, _, half, _ = sizes
    keep[:, tile_of(half)] = row_mass[...] * (1.0 / narrow) - gather_rows(state[0])
    keep[:, tile_of(half + 1)] = down(state[1])


def open_kernel(sizes, *refs):
    narrow, base, half, chips = sizes
    sources, targets, (give, keep, weight, row_all, sems) = refs[:6], refs[6:12], refs[12:]
    cost, plan, row_mass, col_mass, row_dual, col_dual = targets
    core = lax.axis_index(CORE)
    tiles = 2 * half // CHUNKS
    weight[...] = jnp.full((GROUP, LANES), base, jnp.float32)
    small = [pltpu.make_async_copy(sources[n], targets[n], sems.at[n, 0]) for n in range(2, 6)]
    for copy in small:
        copy.start()
    firsts, copies = [], []
    for k in range(CHUNKS):
        side = 1 - core if k < CHUNKS // 2 else core
        firsts.append(side * half + (k % (CHUNKS // 2)) * tiles)
        lanes = span(firsts[k], tiles)
        for n in range(2):
            copy = pltpu.make_async_copy(
                sources[n].at[:, lanes], targets[n].at[:, lanes], sems.at[n, k]
            )
            copy.start()
            copies.append(copy)
    for copy in small:
        copy.wait()
    spread_rows(row_dual[...], row_all)
    state = zeros(row_all)
    for k in range(CHUNKS):
        copies[2 * k].wait()
        copies[2 * k + 1].wait()
        target = give if k < CHUNKS // 2 else keep
        shift = (k % (CHUNKS // 2)) * tiles
        put = into(target, col_mass, 2 * chips)
        state = sweep(
            jnp.float32(1.0), cost, plan, plan, row_all, col_dual, (firsts[k], tiles), state,
            lambda n, j, cols, put=put, shift=shift: put(n + shift, j, cols),
        )
    tail(keep, row_mass, state, sizes)


def middle_kernel(
    sizes, mine, theirs, own_row, weight, cost, plan, row_mass, col_mass, row_dual, col_dual,
    fresh_plan, give, keep, new_weight, new_row, new_col, row_all,
):
    narrow, base, half, chips = sizes
    core = lax.axis_index(CORE)
    step = dual_update(
        mine, theirs, own_row, weight, row_dual, col_dual, new_weight, new_row, new_col, sizes
    )
    spread_rows(new_row[...], row_all)
    state = zeros(row_all)
    for side, target in ((1 - core, give), (core, keep)):
        state = sweep(
            step, cost, plan, fresh_plan, row_all, new_col, (side * half, half), state,
            into(target, col_mass, 2 * chips),
        )
    tail(keep, row_mass, state, sizes)


def close_kernel(
    sizes, mine, theirs, own_row, weight, cost, plan, row_mass, col_mass, row_dual, col_dual,
    plan_out, sent, row_sent, new_weight, new_row, new_col, row_all, fresh_plan, sems,
):
    narrow, base, half, chips = sizes
    step = dual_update(
        mine, theirs, own_row, weight, row_dual, col_dual, new_weight, new_row, new_col, sizes
    )
    spread_rows(new_row[...], row_all)
    state = zeros(row_all)

    def done(n, j, cols):
        share = col_mass[:, span(j, 1)] * (1.0 / (2 * chips)) - cols
        for p in range(2 * chips):
            sent[p, pl.ds(j, 1), :] = share

    tiles = 2 * half // CHUNKS
    copies = []
    for k in range(CHUNKS):
        state = sweep(
            step, cost, plan, fresh_plan, row_all, new_col, (k * tiles, tiles), state, done
        )
        lanes = tile_of(k * tiles, tiles)
        copy = pltpu.make_async_copy(fresh_plan.at[:, lanes], plan_out.at[:, lanes], sems.at[k])
        copy.start()
        copies.append(copy)
    row_sent[...] = row_mass[...] * (1.0 / narrow) - gather_rows(state[0])
    for copy in copies:
        copy.wait()


def build_kernel(sizes, keep, came, sent):
    half = sizes[2]
    cols = keep[:, tile_of(0, half)] + came[...]
    rest = keep[:, tile_of(half, 2)]
    for p in range(sent.shape[0]):
        sent[p, :, tile_of(0, half)] = cols
        sent[p, :, tile_of(half, 2)] = rest


def reduce_kernel(sizes, got, mine, own_row, held, rows_held):
    narrow, base, half, chips = sizes
    column = lax.axis_index("narrow")
    place = lax.axis_index("wide_0") * lax.axis_size("wide_1") + lax.axis_index("wide_1")
    col_squares = jnp.zeros((1, half * LANES), jnp.float32)
    moved = jnp.zeros((1, LANES), jnp.float32)
    for n in range(narrow):
        cols = got[n]
        for p in range(1, chips):
            cols = cols + got[p * narrow + n]
        moved = moved + cols[:, tile_of(half + 1)]
        cols = cols[:, tile_of(0, half)]
        held[n] = cols
        col_squares = col_squares + cols * cols
    squares = jnp.zeros((1, LANES), jnp.float32)
    for r in range(half):
        squares = squares + col_squares[:, tile_of(r)]
    for p in range(chips):
        row = got[p * narrow, :, tile_of(half)]
        for n in range(1, narrow):
            row = row + got[p * narrow + n, :, tile_of(half)]
        rows_held[p] = row
        squares = squares + row * row
    mine[:, tile_of(0, half)] = held[column]
    mine[:, tile_of(half)] = squares
    mine[:, tile_of(half + 1)] = moved
    own_row[...] = rows_held[place]


def finish_kernel(sizes, got, row_got, weight, row_dual, col_dual, row_out, col_out):
    narrow, base, half, chips = sizes
    step = base * weight[0:1, :]
    rows = row_got[0]
    for n in range(1, narrow):
        rows = rows + row_got[n]
    row_out[...] = row_dual[...] + step * rows
    cols = got[0]
    for p in range(1, 2 * chips):
        cols = cols + got[p]
    for j in range(2 * half):
        col_out[:, tile_of(j)] = col_dual[:, tile_of(j)] + step * cols[j : j + 1, :]


VM = pl.BlockSpec(memory_space=pltpu.VMEM)
HB = pl.BlockSpec(memory_space=pltpu.HBM)
ROOM = pltpu.CompilerParams(vmem_limit_bytes=16 << 20)


def shards(cost, plan, row_mass, col_mass, row_dual, col_dual):
    rows, cols = plan.shape
    tiles = cols // LANES
    half = tiles // 2
    narrow = lax.axis_size("narrow")
    wide = lax.axis_size(WIDE)
    chips = wide // 2
    base = 0.9 / math.sqrt(rows * wide + cols * narrow)
    sizes = (narrow, base, half, chips)
    row_mass, row_dual = row_mass.reshape(1, rows), row_dual.reshape(1, rows)
    col_mass, col_dual = col_mass.reshape(1, cols), col_dual.reshape(1, cols)

    def vm(*shape):
        return pltpu.VMEM(shape, jnp.float32)

    def near(*arrays):
        return [pltpu.with_memory_space_constraint(array, pltpu.VMEM) for array in arrays]

    big, state, one, many = vm(rows, cols), vm(GROUP, LANES), vm(1, rows), vm(1, cols)
    give, keep = vm(1, half * LANES), vm(1, (half + 2) * LANES)
    spread = vm(rows, LANES)

    inputs = (cost, plan, row_mass, col_mass, row_dual, col_dual)
    *held, given, kept, weight = pl.pallas_call(
        functools.partial(open_kernel, sizes),
        out_shape=(big, big, one, many, one, many, give, keep, state),
        in_specs=[HB] * 6,
        out_specs=(VM,) * 9,
        scratch_shapes=[spread, pltpu.SemaphoreType.DMA((6, CHUNKS))],
        compiler_params=ROOM,
        name="open_step",
    )(*(pltpu.with_memory_space_constraint(array, pltpu.HBM) for array in inputs))
    cost, plan, row_mass, col_mass, row_dual, col_dual = held
    for step in range(1, ITERS):
        came = swap(given)
        sent = pl.pallas_call(
            functools.partial(build_kernel, sizes),
            out_shape=vm(chips * narrow, 1, (half + 2) * LANES),
            in_specs=[VM] * 2,
            out_specs=VM,
            compiler_params=ROOM,
            name="build_step",
        )(*near(kept, came))
        got = exchange(sent, CHIPS)
        mine, own_row = pl.pallas_call(
            functools.partial(reduce_kernel, sizes),
            out_shape=(keep, one),
            in_specs=[VM],
            out_specs=(VM, VM),
            scratch_shapes=[vm(narrow, 1, half * LANES), vm(chips, 1, rows)],
            compiler_params=ROOM,
            name="reduce_step",
        )(*near(got))
        theirs = swap(mine)
        operands = near(
            mine, theirs, own_row, weight, cost, plan, row_mass, col_mass, row_dual, col_dual
        )
        if step < ITERS - 1:
            plan, given, kept, weight, row_dual, col_dual = pl.pallas_call(
                functools.partial(middle_kernel, sizes),
                out_shape=(big, give, keep, state, one, many),
                in_specs=[VM] * 10,
                out_specs=(VM,) * 6,
                scratch_shapes=[spread],
                compiler_params=ROOM,
                name="middle_step",
            )(*operands)
        else:
            plan, sent, row_sent, weight, row_dual, col_dual = pl.pallas_call(
                functools.partial(close_kernel, sizes),
                out_shape=(
                    jax.ShapeDtypeStruct((rows, cols), jnp.float32),
                    vm(wide, tiles, LANES), one, state, one, many,
                ),
                in_specs=[VM] * 10,
                out_specs=(HB,) + (VM,) * 5,
                scratch_shapes=[spread, big, pltpu.SemaphoreType.DMA((CHUNKS,))],
                compiler_params=ROOM,
                name="close_step",
            )(*operands)
    got = exchange(sent, WIDE)
    row_got = lax.all_gather(row_sent, "narrow")
    row_dual, col_dual = pl.pallas_call(
        functools.partial(finish_kernel, sizes),
        out_shape=tuple(jax.ShapeDtypeStruct(s.shape, s.dtype) for s in (one, many)),
        in_specs=[VM] * 5,
        out_specs=(VM, VM),
        compiler_params=ROOM,
        name="finish_step",
    )(*near(got), row_got, weight, row_dual, col_dual)
    return (plan, row_dual.reshape(rows), col_dual.reshape(cols))


def solution(mesh):
    split = Mesh(
        mesh.devices.reshape(4, 4, 2, mesh.shape["narrow"]),
        ("wide_0", "wide_1", "wide_2", "narrow"),
    )
    placed = (P(WIDE, "narrow"), P(WIDE, "narrow"), P(WIDE), P("narrow"), P(WIDE), P("narrow"))
    return jax.shard_map(
        shards,
        mesh=split,
        in_specs=placed,
        out_specs=(P(WIDE, "narrow"), P(WIDE), P("narrow")),
        check_vma=False,
    )
```

```python
import functools
import math

import jax
import jax.numpy as jnp
from jax import lax
from jax.experimental import pallas as pl
from jax.experimental.pallas import tpu as pltpu
from jax.sharding import Mesh
from jax.sharding import PartitionSpec as P

ITERS = 4
LANES = 128
GROUP = 8
CHUNKS = 4
CORE = "wide_2"
WIDE = ("wide_0", "wide_1", "wide_2")
CHIPS = ("wide_1", "narrow", "wide_0")
PLANE = ("wide_1", "wide_0")


def exchange(array, axes):
    return lax.all_to_all(array, axes, split_axis=0, concat_axis=0, tiled=True)


def swap(array):
    return lax.ppermute(array, CORE, [(0, 1), (1, 0)])


def total(block):
    return jnp.sum(jnp.sum(block, axis=0, keepdims=True), axis=1, keepdims=True)


def down(block):
    return jnp.sum(block, axis=0, keepdims=True)


def span(start, size):
    return pl.ds(pl.multiple_of(start * LANES, LANES), size * LANES)


def tile_of(n, size=1):
    return slice(n * LANES, (n + size) * LANES)


def dual_update(mine, theirs, own_row, weight, row_dual, col_dual, new_weight, new_row, new_col, sizes):
    base, half = sizes[1], sizes[2]
    core = lax.axis_index(CORE)
    left_square = total(mine[:, tile_of(half)]) + total(theirs[:, tile_of(half)])
    moved = total(mine[:, tile_of(half + 1)]) + total(theirs[:, tile_of(half + 1)])
    old = weight[...]
    dual_step = base * old
    dual_moved = dual_step * dual_step * left_square
    fresh_weight = jnp.sqrt(old * jnp.sqrt((dual_moved + 1.0) / (moved + 1.0)))
    new_weight[...] = fresh_weight
    new_row[...] = row_dual[...] + dual_step[0:1, :] * own_row[...]
    scale = jnp.broadcast_to(dual_step[0:1, 0:1], (1, half * LANES))
    for side, part in ((core, mine), (1 - core, theirs)):
        lanes = span(side * half, half)
        new_col[:, lanes] = col_dual[:, lanes] + scale * part[:, tile_of(0, half)]
    return base / fresh_weight


def sweep(step, cost, plan, fresh_plan, row_all, col_dual, tiles, state, done):
    first, count = tiles
    groups = len(state[0])

    def tile(n, state):
        rows, moved = list(state[0]), state[1]
        j = first + n
        lanes = span(j, 1)
        col = jnp.broadcast_to(col_dual[:, lanes], (GROUP, LANES))
        cols = None
        for g in range(groups):
            part = slice(g * GROUP, (g + 1) * GROUP)
            old = plan[part, lanes]
            gap = cost[part, lanes] - row_all[part, :] - col
            fresh = jnp.maximum(old - step * gap, 0.0)
            change = fresh - old
            extrap = fresh + change
            fresh_plan[part, lanes] = fresh
            rows[g] = rows[g] + extrap
            cols = extrap if cols is None else cols + extrap
            moved = moved + change * change
        done(n, j, down(cols))
        return tuple(rows), moved

    return lax.fori_loop(0, count, tile, state, unroll=2)


def spread_rows(row_dual, row_all):
    row_all[...] = jnp.transpose(jnp.broadcast_to(row_dual, (LANES, LANES)))


def gather_rows(rows):
    return down(jnp.transpose(jnp.concatenate(rows, axis=0)))


def zeros(row_all):
    zero = jnp.zeros((GROUP, LANES), jnp.float32)
    return tuple(zero for _ in range(row_all.shape[0] // GROUP)), zero


def into(target, col_mass, wide):
    def done(n, j, cols):
        target[:, span(n, 1)] = col_mass[:, span(j, 1)] * (1.0 / wide) - cols

    return done


def tail(keep, row_mass, state, sizes):
    narrow, _, half, _ = sizes
    keep[:, tile_of(half)] = row_mass[...] * (1.0 / narrow) - gather_rows(state[0])
    keep[:, tile_of(half + 1)] = down(state[1])


def open_kernel(sizes, *refs):
    narrow, base, half, chips = sizes
    sources, targets, (give, keep, weight, row_all, sems) = refs[:6], refs[6:12], refs[12:]
    cost, plan, row_mass, col_mass, row_dual, col_dual = targets
    core = lax.axis_index(CORE)
    tiles = 2 * half // CHUNKS
    weight[...] = jnp.full((GROUP, LANES), base, jnp.float32)
    small = [pltpu.make_async_copy(sources[n], targets[n], sems.at[n, 0]) for n in range(2, 6)]
    for copy in small:
        copy.start()
    firsts, copies = [], []
    for k in range(CHUNKS):
        side = 1 - core if k < CHUNKS // 2 else core
        firsts.append(side * half + (k % (CHUNKS // 2)) * tiles)
        lanes = span(firsts[k], tiles)
        for n in range(2):
            copy = pltpu.make_async_copy(
                sources[n].at[:, lanes], targets[n].at[:, lanes], sems.at[n, k]
            )
            copy.start()
            copies.append(copy)
    for copy in small:
        copy.wait()
    spread_rows(row_dual[...], row_all)
    state = zeros(row_all)
    for k in range(CHUNKS):
        copies[2 * k].wait()
        copies[2 * k + 1].wait()
        target = give if k < CHUNKS // 2 else keep
        shift = (k % (CHUNKS // 2)) * tiles
        put = into(target, col_mass, 2 * chips)
        state = sweep(
            jnp.float32(1.0), cost, plan, plan, row_all, col_dual, (firsts[k], tiles), state,
            lambda n, j, cols, put=put, shift=shift: put(n + shift, j, cols),
        )
    tail(keep, row_mass, state, sizes)


def give_kernel(
    sizes, mine, theirs, own_row, weight, cost, plan, col_mass, row_dual, col_dual,
    fresh_plan, give, row_sums, moved_sums, row_all, new_weight, new_row, new_col,
):
    _, _, half, chips = sizes
    step = dual_update(
        mine, theirs, own_row, weight, row_dual, col_dual, new_weight, new_row, new_col, sizes
    )
    spread_rows(new_row[...], row_all)
    side = 1 - lax.axis_index(CORE)
    rows, moved = sweep(
        step, cost, plan, fresh_plan, row_all, new_col, (side * half, half), zeros(row_all),
        into(give, col_mass, 2 * chips),
    )
    row_sums[...] = jnp.concatenate(rows, axis=0)
    moved_sums[...] = moved


def keep_kernel(
    sizes, weight, cost, plan, row_mass, col_mass, row_all, col_dual, row_sums, moved_sums,
    fresh_plan, keep, row_share,
):
    _, base, half, chips = sizes
    side = lax.axis_index(CORE)
    rows = row_sums[...]
    groups = row_all.shape[0] // GROUP
    state = tuple(rows[g * GROUP : (g + 1) * GROUP] for g in range(groups)), moved_sums[...]
    state = sweep(
        base / weight[...], cost, plan, fresh_plan, row_all, col_dual, (side * half, half), state,
        into(keep, col_mass, 2 * chips),
    )
    tail(keep, row_mass, state, sizes)
    row_share[...] = keep[:, tile_of(half)]


def build_kernel(sizes, keep, came, sent):
    half = sizes[2]
    cols = keep[:, tile_of(0, half)] + came[...]
    rest = keep[:, tile_of(half, 2)]
    for p in range(sent.shape[0]):
        sent[p, :, tile_of(0, half)] = cols
        sent[p, :, tile_of(half, 2)] = rest


def reduce_kernel(sizes, got, mine, own_row, held, rows_held):
    narrow, base, half, chips = sizes
    column = lax.axis_index("narrow")
    across, along = lax.axis_index("wide_0"), lax.axis_index("wide_1")
    wide_0 = lax.axis_size("wide_0")
    peers = [
        [(b * narrow + n) * wide_0 + a for b in range(chips // wide_0) for a in range(wide_0)]
        for n in range(narrow)
    ]
    col_squares = jnp.zeros((1, half * LANES), jnp.float32)
    moved = jnp.zeros((1, LANES), jnp.float32)
    for n in range(narrow):
        cols = got[peers[n][0]]
        for p in peers[n][1:]:
            cols = cols + got[p]
        moved = moved + cols[:, tile_of(half + 1)]
        cols = cols[:, tile_of(0, half)]
        held[n] = cols
        col_squares = col_squares + cols * cols
    squares = jnp.zeros((1, LANES), jnp.float32)
    for r in range(half):
        squares = squares + col_squares[:, tile_of(r)]
    for p in range(chips):
        row = got[peers[0][p], :, tile_of(half)]
        for n in range(1, narrow):
            row = row + got[peers[n][p], :, tile_of(half)]
        rows_held[p] = row
        squares = squares + row * row
    mine[:, tile_of(0, half)] = held[column]
    mine[:, tile_of(half)] = squares
    mine[:, tile_of(half + 1)] = moved
    own_row[...] = rows_held[along * wide_0 + across]


def last_build_kernel(sizes, keep, came, sent):
    cols = keep[:, tile_of(0, sizes[2])] + came[...]
    for p in range(sent.shape[0]):
        sent[p] = cols


def store_kernel(plan, plan_out, stored, sem):
    copy = pltpu.make_async_copy(plan, plan_out, sem)
    copy.start()
    stored[...] = jnp.zeros_like(stored)
    copy.wait()


def last_reduce_kernel(sizes, got, row_got, stored, mine, row_left):
    cols = got[0]
    for p in range(1, got.shape[0]):
        cols = cols + got[p]
    mine[...] = cols
    rows = row_got[0]
    for n in range(1, row_got.shape[0]):
        rows = rows + row_got[n]
    row_left[...] = rows


def finish_kernel(sizes, mine, theirs, row_left, weight, row_dual, col_dual, row_out, col_out):
    _, base, half, _ = sizes
    core = lax.axis_index(CORE)
    step = base * weight[0:1, :]
    row_out[...] = row_dual[...] + step * row_left[...]
    scale = jnp.broadcast_to(step[:, 0:1], (1, half * LANES))
    for side, part in ((core, mine), (1 - core, theirs)):
        lanes = span(side * half, half)
        col_out[:, lanes] = col_dual[:, lanes] + scale * part[...]


VM = pl.BlockSpec(memory_space=pltpu.VMEM)
HB = pl.BlockSpec(memory_space=pltpu.HBM)
ROOM = pltpu.CompilerParams(vmem_limit_bytes=16 << 20)


def shards(cost, plan, row_mass, col_mass, row_dual, col_dual):
    rows, cols = plan.shape
    tiles = cols // LANES
    half = tiles // 2
    narrow = lax.axis_size("narrow")
    wide = lax.axis_size(WIDE)
    chips = wide // 2
    base = 0.9 / math.sqrt(rows * wide + cols * narrow)
    sizes = (narrow, base, half, chips)
    row_mass, row_dual = row_mass.reshape(1, rows), row_dual.reshape(1, rows)
    col_mass, col_dual = col_mass.reshape(1, cols), col_dual.reshape(1, cols)

    def vm(*shape):
        return pltpu.VMEM(shape, jnp.float32)

    def near(*arrays):
        return [pltpu.with_memory_space_constraint(array, pltpu.VMEM) for array in arrays]

    big, state, one, many = vm(rows, cols), vm(GROUP, LANES), vm(1, rows), vm(1, cols)
    give, keep = vm(1, half * LANES), vm(1, (half + 2) * LANES)
    spread = vm(rows, LANES)

    inputs = (cost, plan, row_mass, col_mass, row_dual, col_dual)
    *held, given, kept, weight = pl.pallas_call(
        functools.partial(open_kernel, sizes),
        out_shape=(big, big, one, many, one, many, give, keep, state),
        in_specs=[HB] * 6,
        out_specs=(VM,) * 9,
        scratch_shapes=[spread, pltpu.SemaphoreType.DMA((6, CHUNKS))],
        compiler_params=ROOM,
        name="open_step",
    )(*(pltpu.with_memory_space_constraint(array, pltpu.HBM) for array in inputs))
    cost, plan, row_mass, col_mass, row_dual, col_dual = held
    work = pl.CostEstimate(flops=6 * rows * cols, bytes_accessed=0, transcendentals=0)
    for step in range(1, ITERS):
        came = swap(given)
        sent = pl.pallas_call(
            functools.partial(build_kernel, sizes),
            out_shape=vm(chips * narrow, 1, (half + 2) * LANES),
            in_specs=[VM] * 2,
            out_specs=VM,
            compiler_params=ROOM,
            name="build_step",
        )(*near(kept, came))
        got = exchange(sent, CHIPS)
        mine, own_row = pl.pallas_call(
            functools.partial(reduce_kernel, sizes),
            out_shape=(keep, one),
            in_specs=[VM],
            out_specs=(VM, VM),
            scratch_shapes=[vm(narrow, 1, half * LANES), vm(chips, 1, rows)],
            compiler_params=ROOM,
            name="reduce_step",
        )(*near(got))
        theirs = swap(mine)
        plan, given, row_sums, moved_sums, row_all, weight, row_dual, col_dual = pl.pallas_call(
            functools.partial(give_kernel, sizes),
            out_shape=(big, give, spread, state, spread, state, one, many),
            in_specs=[VM] * 9,
            out_specs=(VM,) * 8,
            input_output_aliases={5: 0},
            compiler_params=ROOM,
            cost_estimate=work,
            name="give_step",
        )(*near(mine, theirs, own_row, weight, cost, plan, col_mass, row_dual, col_dual))
        plan, kept, row_sent = pl.pallas_call(
            functools.partial(keep_kernel, sizes),
            out_shape=(big, keep, one),
            in_specs=[VM] * 9,
            out_specs=(VM,) * 3,
            input_output_aliases={2: 0},
            compiler_params=ROOM,
            cost_estimate=work,
            name="keep_step",
        )(*near(weight, cost, plan, row_mass, col_mass, row_all, col_dual, row_sums, moved_sums))
    came = swap(given)
    sent = pl.pallas_call(
        functools.partial(last_build_kernel, sizes),
        out_shape=vm(chips, 1, half * LANES),
        in_specs=[VM] * 2,
        out_specs=VM,
        compiler_params=ROOM,
        name="last_build_step",
    )(*near(kept, came))
    got = exchange(sent, PLANE)
    row_got = lax.all_gather(row_sent, "narrow")
    plan, stored = pl.pallas_call(
        store_kernel,
        out_shape=(jax.ShapeDtypeStruct((rows, cols), jnp.float32), one),
        in_specs=[VM],
        out_specs=(HB, VM),
        scratch_shapes=[pltpu.SemaphoreType.DMA],
        compiler_params=ROOM,
        cost_estimate=work,
        name="store_step",
    )(*near(plan))
    mine, row_left = pl.pallas_call(
        functools.partial(last_reduce_kernel, sizes),
        out_shape=(give, one),
        in_specs=[VM] * 3,
        out_specs=(VM, VM),
        compiler_params=ROOM,
        name="last_reduce_step",
    )(*near(got, row_got, stored))
    theirs = swap(mine)
    row_dual, col_dual = pl.pallas_call(
        functools.partial(finish_kernel, sizes),
        out_shape=tuple(jax.ShapeDtypeStruct(s.shape, s.dtype) for s in (one, many)),
        in_specs=[VM] * 6,
        out_specs=(VM, VM),
        compiler_params=ROOM,
        name="finish_step",
    )(*near(mine, theirs, row_left, weight, row_dual, col_dual))
    return (plan, row_dual.reshape(rows), col_dual.reshape(cols))


def solution(mesh):
    split = Mesh(
        mesh.devices.reshape(4, 4, 2, mesh.shape["narrow"]),
        ("wide_0", "wide_1", "wide_2", "narrow"),
    )
    placed = (P(WIDE, "narrow"), P(WIDE, "narrow"), P(WIDE), P("narrow"), P(WIDE), P("narrow"))
    return jax.shard_map(
        shards,
        mesh=split,
        in_specs=placed,
        out_specs=(P(WIDE, "narrow"), P(WIDE), P("narrow")),
        check_vma=False,
    )
```

```python
import functools
import math

import jax
import jax.numpy as jnp
from jax import lax
from jax.experimental import pallas as pl
from jax.experimental.pallas import tpu as pltpu
from jax.sharding import Mesh
from jax.sharding import PartitionSpec as P

ITERS = 4
LANES = 128
GROUP = 8
CHUNKS = 4
CORE = "wide_2"
WIDE = ("wide_0", "wide_1", "wide_2")
COLUMN = ("wide_2", "narrow")
PLANE = ("wide_0", "wide_1")


def exchange(array, axes):
    return lax.all_to_all(array, axes, split_axis=0, concat_axis=0, tiled=True)


def swap(array):
    return lax.ppermute(array, CORE, [(0, 1), (1, 0)])


def total(block):
    return jnp.sum(jnp.sum(block, axis=0, keepdims=True), axis=1, keepdims=True)


def down(block):
    return jnp.sum(block, axis=0, keepdims=True)


def span(start, size):
    return pl.ds(pl.multiple_of(start * LANES, LANES), size * LANES)


def tile_of(n, size=1):
    return slice(n * LANES, (n + size) * LANES)


def dual_update(
    got, weight, row_dual, col_dual, new_weight, new_row, new_col, rows_held, sizes
):
    narrow, base, half, chips = sizes
    core = lax.axis_index(CORE)
    place = lax.axis_index("wide_0") * lax.axis_size("wide_1") + lax.axis_index("wide_1")
    squares, rest = None, None
    for c in range(2):
        rows, other = got[c * narrow, :, tile_of(half, chips)], got[c * narrow, :, tile_of(half + chips, 2)]
        for n in range(c * narrow + 1, (c + 1) * narrow):
            rows = rows + got[n, :, tile_of(half, chips)]
            other = other + got[n, :, tile_of(half + chips, 2)]
        rows_held[c] = rows
        squares = rows * rows if squares is None else squares + rows * rows
        rest = other if rest is None else rest + other
    left_square = total(squares) + total(rest[:, tile_of(0)])
    moved = total(rest[:, tile_of(1)])
    old = weight[...]
    dual_step = base * old
    dual_moved = dual_step * dual_step * left_square
    fresh_weight = jnp.sqrt(old * jnp.sqrt((dual_moved + 1.0) / (moved + 1.0)))
    new_weight[...] = fresh_weight
    new_row[...] = row_dual[...] + dual_step[0:1, :] * rows_held[core, :, span(place, 1)]
    scale = jnp.broadcast_to(dual_step[0:1, 0:1], (1, half * LANES))
    column = lax.axis_index("narrow")
    for c in range(2):
        lanes = tile_of(c * half, half)
        new_col[:, lanes] = col_dual[:, lanes] + scale * got[c * narrow + column, :, tile_of(0, half)]
    return base / fresh_weight


def sweep(step, cost, plan, fresh_plan, row_all, col_dual, tiles, state, done):
    first, count = tiles
    groups = len(state[0])

    def tile(n, state):
        rows, moved = list(state[0]), state[1]
        j = first + n
        lanes = span(j, 1)
        col = jnp.broadcast_to(col_dual[:, lanes], (GROUP, LANES))
        cols = None
        for g in range(groups):
            part = slice(g * GROUP, (g + 1) * GROUP)
            old = plan[part, lanes]
            gap = cost[part, lanes] - row_all[part, :] - col
            fresh = jnp.maximum(old - step * gap, 0.0)
            change = fresh - old
            extrap = fresh + change
            fresh_plan[part, lanes] = fresh
            rows[g] = rows[g] + extrap
            cols = extrap if cols is None else cols + extrap
            moved = moved + change * change
        done(n, j, down(cols))
        return tuple(rows), moved

    return lax.fori_loop(0, count, tile, state, unroll=2)


def spread_rows(row_dual, row_all):
    row_all[...] = jnp.transpose(jnp.broadcast_to(row_dual, (LANES, LANES)))


def gather_rows(rows):
    return down(jnp.transpose(jnp.concatenate(rows, axis=0)))


def zeros(row_all):
    zero = jnp.zeros((GROUP, LANES), jnp.float32)
    return tuple(zero for _ in range(row_all.shape[0] // GROUP)), zero


def into(target, col_mass, wide):
    def done(n, j, cols):
        target[:, span(n, 1)] = col_mass[:, span(j, 1)] * (1.0 / wide) - cols

    return done


def tail(keep, row_mass, state, sizes):
    narrow, _, half, _ = sizes
    keep[:, tile_of(half)] = row_mass[...] * (1.0 / narrow) - gather_rows(state[0])
    keep[:, tile_of(half + 1)] = down(state[1])


def open_kernel(sizes, *refs):
    narrow, base, half, chips = sizes
    sources, targets, (give, keep, weight, row_all, sems) = refs[:6], refs[6:12], refs[12:]
    cost, plan, row_mass, col_mass, row_dual, col_dual = targets
    core = lax.axis_index(CORE)
    tiles = 2 * half // CHUNKS
    weight[...] = jnp.full((GROUP, LANES), base, jnp.float32)
    small = [pltpu.make_async_copy(sources[n], targets[n], sems.at[n, 0]) for n in range(2, 6)]
    for copy in small:
        copy.start()
    firsts, copies = [], []
    for k in range(CHUNKS):
        side = 1 - core if k < CHUNKS // 2 else core
        firsts.append(side * half + (k % (CHUNKS // 2)) * tiles)
        lanes = span(firsts[k], tiles)
        for n in range(2):
            copy = pltpu.make_async_copy(
                sources[n].at[:, lanes], targets[n].at[:, lanes], sems.at[n, k]
            )
            copy.start()
            copies.append(copy)
    for copy in small:
        copy.wait()
    spread_rows(row_dual[...], row_all)
    state = zeros(row_all)
    for k in range(CHUNKS):
        copies[2 * k].wait()
        copies[2 * k + 1].wait()
        target = give if k < CHUNKS // 2 else keep
        shift = (k % (CHUNKS // 2)) * tiles
        put = into(target, col_mass, 2 * chips)
        state = sweep(
            jnp.float32(1.0), cost, plan, plan, row_all, col_dual, (firsts[k], tiles), state,
            lambda n, j, cols, put=put, shift=shift: put(n + shift, j, cols),
        )
    tail(keep, row_mass, state, sizes)


def give_kernel(
    sizes, got, weight, cost, plan, col_mass, row_dual, col_dual,
    fresh_plan, give, row_sums, moved_sums, row_all, new_weight, new_row, new_col, rows_held,
):
    _, _, half, chips = sizes
    step = dual_update(
        got, weight, row_dual, col_dual, new_weight, new_row, new_col, rows_held, sizes
    )
    spread_rows(new_row[...], row_all)
    side = 1 - lax.axis_index(CORE)
    rows, moved = sweep(
        step, cost, plan, fresh_plan, row_all, new_col, (side * half, half), zeros(row_all),
        into(give, col_mass, 2 * chips),
    )
    row_sums[...] = jnp.concatenate(rows, axis=0)
    moved_sums[...] = moved


def keep_kernel(
    sizes, weight, cost, plan, half_plan, row_mass, col_mass, row_all, col_dual, row_sums,
    moved_sums, fresh_plan, keep, row_share,
):
    _, base, half, chips = sizes
    side = lax.axis_index(CORE)
    rows = row_sums[...]
    groups = row_all.shape[0] // GROUP
    state = tuple(rows[g * GROUP : (g + 1) * GROUP] for g in range(groups)), moved_sums[...]
    state = sweep(
        base / weight[...], cost, plan, fresh_plan, row_all, col_dual, (side * half, half), state,
        into(keep, col_mass, 2 * chips),
    )
    tail(keep, row_mass, state, sizes)
    row_share[...] = keep[:, tile_of(half)]


def build_kernel(sizes, keep, came, sent):
    half = sizes[2]
    cols = keep[:, tile_of(0, half)] + came[...]
    rest = keep[:, tile_of(half, 2)]
    for p in range(sent.shape[0]):
        sent[p, :, tile_of(0, half)] = cols
        sent[p, :, tile_of(half, 2)] = rest


def reduce_kernel(sizes, got, sent):
    narrow, base, half, chips = sizes
    cols = got[0]
    for p in range(1, chips):
        cols = cols + got[p]
    moved = cols[:, tile_of(half + 1)]
    cols = cols[:, tile_of(0, half)]
    sent[0, :, tile_of(0, half)] = cols
    cols = cols * cols
    squares = cols[:, tile_of(0)]
    for r in range(1, half):
        squares = squares + cols[:, tile_of(r)]
    for p in range(chips):
        sent[0, :, tile_of(half + p)] = got[p, :, tile_of(half)]
    sent[0, :, tile_of(half + chips)] = squares
    sent[0, :, tile_of(half + chips + 1)] = moved
    everything = sent[0]
    for q in range(1, sent.shape[0]):
        sent[q] = everything


def last_build_kernel(sizes, keep, came, sent):
    cols = keep[:, tile_of(0, sizes[2])] + came[...]
    for p in range(sent.shape[0]):
        sent[p] = cols


def store_kernel(plan, plan_out, stored, sem):
    copy = pltpu.make_async_copy(plan, plan_out, sem)
    copy.start()
    stored[...] = jnp.zeros_like(stored)
    copy.wait()


def last_reduce_kernel(sizes, got, row_got, stored, mine, row_left):
    cols = got[0]
    for p in range(1, got.shape[0]):
        cols = cols + got[p]
    mine[...] = cols
    rows = row_got[0]
    for n in range(1, row_got.shape[0]):
        rows = rows + row_got[n]
    row_left[...] = rows


def finish_kernel(sizes, mine, theirs, row_left, weight, row_dual, col_dual, row_out, col_out):
    _, base, half, _ = sizes
    core = lax.axis_index(CORE)
    step = base * weight[0:1, :]
    row_out[...] = row_dual[...] + step * row_left[...]
    scale = jnp.broadcast_to(step[:, 0:1], (1, half * LANES))
    for side, part in ((core, mine), (1 - core, theirs)):
        lanes = span(side * half, half)
        col_out[:, lanes] = col_dual[:, lanes] + scale * part[...]


VM = pl.BlockSpec(memory_space=pltpu.VMEM)
HB = pl.BlockSpec(memory_space=pltpu.HBM)
ROOM = pltpu.CompilerParams(vmem_limit_bytes=16 << 20)


def shards(cost, plan, row_mass, col_mass, row_dual, col_dual):
    rows, cols = plan.shape
    tiles = cols // LANES
    half = tiles // 2
    narrow = lax.axis_size("narrow")
    wide = lax.axis_size(WIDE)
    chips = wide // 2
    base = 0.9 / math.sqrt(rows * wide + cols * narrow)
    sizes = (narrow, base, half, chips)
    row_mass, row_dual = row_mass.reshape(1, rows), row_dual.reshape(1, rows)
    col_mass, col_dual = col_mass.reshape(1, cols), col_dual.reshape(1, cols)

    def vm(*shape):
        return pltpu.VMEM(shape, jnp.float32)

    def near(*arrays):
        return [pltpu.with_memory_space_constraint(array, pltpu.VMEM) for array in arrays]

    big, state, one, many = vm(rows, cols), vm(GROUP, LANES), vm(1, rows), vm(1, cols)
    give, keep = vm(1, half * LANES), vm(1, (half + 2) * LANES)
    spread = vm(rows, LANES)

    inputs = (cost, plan, row_mass, col_mass, row_dual, col_dual)
    *held, given, kept, weight = pl.pallas_call(
        functools.partial(open_kernel, sizes),
        out_shape=(big, big, one, many, one, many, give, keep, state),
        in_specs=[HB] * 6,
        out_specs=(VM,) * 9,
        scratch_shapes=[spread, pltpu.SemaphoreType.DMA((6, CHUNKS))],
        compiler_params=ROOM,
        name="open_step",
    )(*(pltpu.with_memory_space_constraint(array, pltpu.HBM) for array in inputs))
    cost, plan, row_mass, col_mass, row_dual, col_dual = held
    work = pl.CostEstimate(flops=6 * rows * cols, bytes_accessed=0, transcendentals=0)
    for step in range(1, ITERS):
        came = swap(given)
        sent = pl.pallas_call(
            functools.partial(build_kernel, sizes),
            out_shape=vm(chips, 1, (half + 2) * LANES),
            in_specs=[VM] * 2,
            out_specs=VM,
            compiler_params=ROOM,
            name="build_step",
        )(*near(kept, came))
        got = exchange(sent, PLANE)
        sent = pl.pallas_call(
            functools.partial(reduce_kernel, sizes),
            out_shape=vm(2 * narrow, 1, (half + chips + 2) * LANES),
            in_specs=[VM],
            out_specs=VM,
            compiler_params=ROOM,
            name="reduce_step",
        )(*near(got))
        got = exchange(sent, COLUMN)
        half_plan, given, row_sums, moved_sums, row_all, weight, row_dual, col_dual = pl.pallas_call(
            functools.partial(give_kernel, sizes),
            out_shape=(big, give, spread, state, spread, state, one, many),
            in_specs=[VM] * 7,
            out_specs=(VM,) * 8,
            scratch_shapes=[vm(2, 1, chips * LANES)],
            compiler_params=ROOM,
            cost_estimate=work,
            name="give_step",
        )(*near(got, weight, cost, plan, col_mass, row_dual, col_dual))
        plan, kept, row_sent = pl.pallas_call(
            functools.partial(keep_kernel, sizes),
            out_shape=(big, keep, one),
            in_specs=[VM] * 10,
            out_specs=(VM,) * 3,
            input_output_aliases={3: 0},
            compiler_params=ROOM,
            cost_estimate=work,
            name="keep_step",
        )(*near(
            weight, cost, plan, half_plan, row_mass, col_mass, row_all, col_dual, row_sums,
            moved_sums,
        ))
    came = swap(given)
    sent = pl.pallas_call(
        functools.partial(last_build_kernel, sizes),
        out_shape=vm(chips, 1, half * LANES),
        in_specs=[VM] * 2,
        out_specs=VM,
        compiler_params=ROOM,
        name="last_build_step",
    )(*near(kept, came))
    got = exchange(sent, PLANE)
    row_got = lax.all_gather(row_sent, "narrow")
    plan, stored = pl.pallas_call(
        store_kernel,
        out_shape=(jax.ShapeDtypeStruct((rows, cols), jnp.float32), one),
        in_specs=[VM],
        out_specs=(HB, VM),
        scratch_shapes=[pltpu.SemaphoreType.DMA],
        compiler_params=ROOM,
        cost_estimate=work,
        name="store_step",
    )(*near(plan))
    mine, row_left = pl.pallas_call(
        functools.partial(last_reduce_kernel, sizes),
        out_shape=(give, one),
        in_specs=[VM] * 3,
        out_specs=(VM, VM),
        compiler_params=ROOM,
        name="last_reduce_step",
    )(*near(got, row_got, stored))
    theirs = swap(mine)
    row_dual, col_dual = pl.pallas_call(
        functools.partial(finish_kernel, sizes),
        out_shape=tuple(jax.ShapeDtypeStruct(s.shape, s.dtype) for s in (one, many)),
        in_specs=[VM] * 6,
        out_specs=(VM, VM),
        compiler_params=ROOM,
        name="finish_step",
    )(*near(mine, theirs, row_left, weight, row_dual, col_dual))
    return (plan, row_dual.reshape(rows), col_dual.reshape(cols))


def solution(mesh):
    split = Mesh(
        mesh.devices.reshape(4, 4, 2, mesh.shape["narrow"]),
        ("wide_0", "wide_1", "wide_2", "narrow"),
    )
    placed = (P(WIDE, "narrow"), P(WIDE, "narrow"), P(WIDE), P("narrow"), P(WIDE), P("narrow"))
    return jax.shard_map(
        shards,
        mesh=split,
        in_specs=placed,
        out_specs=(P(WIDE, "narrow"), P(WIDE), P("narrow")),
        check_vma=False,
    )
```

```python
import functools
import math

import jax
import jax.numpy as jnp
from jax import lax
from jax.experimental import pallas as pl
from jax.experimental.pallas import tpu as pltpu
from jax.sharding import Mesh
from jax.sharding import PartitionSpec as P

ITERS = 4
LANES = 128
GROUP = 8
CHUNKS = 2
WIDTH = 2
MOVED = 2
CORE = "wide_2"
WIDE = ("wide_0", "wide_1", "wide_2")
COLUMN = ("wide_2", "narrow")
PLANE = ("wide_0", "wide_1")


def exchange(array, axes):
    return lax.all_to_all(array, axes, split_axis=0, concat_axis=0, tiled=True)


def swap(array):
    return lax.ppermute(array, CORE, [(0, 1), (1, 0)])


def total(block):
    return jnp.sum(jnp.sum(block, axis=0, keepdims=True), axis=1, keepdims=True)


def down(block):
    return jnp.sum(block, axis=0, keepdims=True)


def span(start, size):
    return pl.ds(pl.multiple_of(start * LANES, LANES), size * LANES)


def tile_of(n, size=1):
    return slice(n * LANES, (n + size) * LANES)


def dual_update(
    got, weight, row_dual, col_dual, new_weight, new_row, new_col, rows_held, sizes
):
    narrow, base, half, chips = sizes
    core = lax.axis_index(CORE)
    place = lax.axis_index("wide_0") * lax.axis_size("wide_1") + lax.axis_index("wide_1")
    squares, rest = None, None
    for c in range(2):
        rows, other = got[c * narrow, :, tile_of(half, chips)], got[c * narrow, :, tile_of(half + chips, 2)]
        for n in range(c * narrow + 1, (c + 1) * narrow):
            rows = rows + got[n, :, tile_of(half, chips)]
            other = other + got[n, :, tile_of(half + chips, 2)]
        rows_held[c] = rows
        squares = rows * rows if squares is None else squares + rows * rows
        rest = other if rest is None else rest + other
    left_square = total(squares) + total(rest[:, tile_of(0)])
    moved = total(rest[:, tile_of(1)])
    old = weight[...]
    dual_step = base * old
    dual_moved = dual_step * dual_step * left_square
    fresh_weight = jnp.sqrt(old * jnp.sqrt((dual_moved + 1.0) / (moved + 1.0)))
    new_weight[...] = fresh_weight
    new_row[...] = row_dual[...] + dual_step[0:1, :] * rows_held[core, :, span(place, 1)]
    scale = jnp.broadcast_to(dual_step[0:1, 0:1], (1, half * LANES))
    column = lax.axis_index("narrow")
    for c in range(2):
        lanes = tile_of(c * half, half)
        new_col[:, lanes] = col_dual[:, lanes] + scale * got[c * narrow + column, :, tile_of(0, half)]
    return base / fresh_weight


def sweep(step, cost, plan, fresh_plan, row_all, col_dual, tiles, state, done):
    first, count = tiles
    groups = len(state[0])

    def some(m, state):
        rows, moved = list(state[0]), list(state[1])
        cols = [[None, None] for _ in range(WIDTH)]
        lanes = [span(first + WIDTH * m + w, 1) for w in range(WIDTH)]
        duals = [jnp.broadcast_to(col_dual[:, lanes[w]], (GROUP, LANES)) for w in range(WIDTH)]
        for g in range(groups):
            part = slice(g * GROUP, (g + 1) * GROUP)
            both = None
            for w in range(WIDTH):
                old = plan[part, lanes[w]]
                gap = cost[part, lanes[w]] - row_all[part, :] - duals[w]
                fresh = jnp.maximum(old - step * gap, 0.0)
                change = fresh - old
                extrap = fresh + change
                fresh_plan[part, lanes[w]] = fresh
                both = extrap if both is None else both + extrap
                sums = cols[w]
                sums[g % 2] = extrap if sums[g % 2] is None else sums[g % 2] + extrap
                at = (g * WIDTH + w) % len(moved)
                moved[at] = moved[at] + change * change
            rows[g] = rows[g] + both
        for w in range(WIDTH):
            done(WIDTH * m + w, first + WIDTH * m + w, down(cols[w][0] + cols[w][1]))
        return tuple(rows), tuple(moved)

    return lax.fori_loop(0, count // WIDTH, some, state)


def spread_rows(row_dual, row_all):
    row_all[...] = jnp.transpose(jnp.broadcast_to(row_dual, (LANES, LANES)))


def gather_rows(rows):
    return down(jnp.transpose(jnp.concatenate(rows, axis=0)))


def zeros(row_all):
    zero = jnp.zeros((GROUP, LANES), jnp.float32)
    return tuple(zero for _ in range(row_all.shape[0] // GROUP)), (zero,) * MOVED


def into(target, col_mass, wide):
    def done(n, j, cols):
        target[:, span(n, 1)] = col_mass[:, span(j, 1)] * (1.0 / wide) - cols

    return done


def tail(keep, row_mass, state, sizes):
    narrow, _, half, _ = sizes
    keep[:, tile_of(half)] = row_mass[...] * (1.0 / narrow) - gather_rows(state[0])
    keep[:, tile_of(half + 1)] = down(sum(state[1][1:], state[1][0]))


def open_kernel(sizes, *refs):
    narrow, base, half, chips = sizes
    sources, targets = refs[:6], refs[6:12]
    fresh_plan, give, row_sums, moved_sums, row_all, weight, sems = refs[12:]
    cost, plan, row_mass, col_mass, row_dual, col_dual = targets
    core = lax.axis_index(CORE)
    tiles = half // CHUNKS
    weight[...] = jnp.full((GROUP, LANES), base, jnp.float32)
    small = [pltpu.make_async_copy(sources[n], targets[n], sems.at[n, 0]) for n in range(2, 6)]
    for copy in small:
        copy.start()
    big = []
    for k in range(CHUNKS + 1):
        first = (1 - core) * half + k * tiles if k < CHUNKS else core * half
        lanes = span(first, tiles if k < CHUNKS else half)
        for n in range(2):
            copy = pltpu.make_async_copy(
                sources[n].at[:, lanes], targets[n].at[:, lanes], sems.at[n, k]
            )
            copy.start()
            big.append(copy)
    for copy in small:
        copy.wait()
    spread_rows(row_dual[...], row_all)
    state = zeros(row_all)
    put = into(give, col_mass, 2 * chips)
    for k in range(CHUNKS):
        big[2 * k].wait()
        big[2 * k + 1].wait()
        shift = k * tiles
        state = sweep(
            jnp.float32(1.0), cost, plan, fresh_plan, row_all, col_dual,
            ((1 - core) * half + shift, tiles), state,
            lambda n, j, cols, shift=shift: put(n + shift, j, cols),
        )
    hold(state, row_sums, moved_sums)
    for copy in big[2 * CHUNKS :]:
        copy.wait()


def hold(state, row_sums, moved_sums):
    row_sums[...] = jnp.concatenate(state[0], axis=0)
    for n in range(MOVED):
        moved_sums[n] = state[1][n]


def give_kernel(
    sizes, got, weight, cost, plan, col_mass, row_dual, col_dual,
    fresh_plan, give, row_sums, moved_sums, row_all, new_weight, new_row, new_col, rows_held,
):
    _, _, half, chips = sizes
    step = dual_update(
        got, weight, row_dual, col_dual, new_weight, new_row, new_col, rows_held, sizes
    )
    spread_rows(new_row[...], row_all)
    side = 1 - lax.axis_index(CORE)
    state = sweep(
        step, cost, plan, fresh_plan, row_all, new_col, (side * half, half), zeros(row_all),
        into(give, col_mass, 2 * chips),
    )
    hold(state, row_sums, moved_sums)


def keep_kernel(
    sizes, weight, cost, plan, half_plan, row_mass, col_mass, row_all, col_dual, row_sums,
    moved_sums, fresh_plan, keep, *row_share,
):
    _, base, half, chips = sizes
    side = lax.axis_index(CORE)
    rows = row_sums[...]
    groups = row_all.shape[0] // GROUP
    state = tuple(rows[g * GROUP : (g + 1) * GROUP] for g in range(groups)), tuple(
        moved_sums[n] for n in range(MOVED)
    )
    state = sweep(
        base / weight[...], cost, plan, fresh_plan, row_all, col_dual, (side * half, half), state,
        into(keep, col_mass, 2 * chips),
    )
    tail(keep, row_mass, state, sizes)
    for share in row_share:
        share[...] = keep[:, tile_of(half)]


def build_kernel(sizes, keep, came, sent):
    half = sizes[2]
    cols = keep[:, tile_of(0, half)] + came[...]
    rest = keep[:, tile_of(half, 2)]
    for p in range(sent.shape[0]):
        sent[p, :, tile_of(0, half)] = cols
        sent[p, :, tile_of(half, 2)] = rest


def reduce_kernel(sizes, got, sent):
    narrow, base, half, chips = sizes
    cols = got[0]
    for p in range(1, chips):
        cols = cols + got[p]
    moved = cols[:, tile_of(half + 1)]
    cols = cols[:, tile_of(0, half)]
    sent[0, :, tile_of(0, half)] = cols
    cols = cols * cols
    squares = cols[:, tile_of(0)]
    for r in range(1, half):
        squares = squares + cols[:, tile_of(r)]
    for p in range(chips):
        sent[0, :, tile_of(half + p)] = got[p, :, tile_of(half)]
    sent[0, :, tile_of(half + chips)] = squares
    sent[0, :, tile_of(half + chips + 1)] = moved
    everything = sent[0]
    for q in range(1, sent.shape[0]):
        sent[q] = everything


def last_build_kernel(sizes, keep, came, sent):
    cols = keep[:, tile_of(0, sizes[2])] + came[...]
    for p in range(sent.shape[0]):
        sent[p] = cols


def store_kernel(plan, after, plan_out, stored, sem):
    copy = pltpu.make_async_copy(plan, plan_out, sem)
    copy.start()
    stored[...] = after[:, tile_of(0)]
    copy.wait()


def last_reduce_kernel(sizes, got, row_got, mine, row_left):
    cols = got[0]
    for p in range(1, got.shape[0]):
        cols = cols + got[p]
    mine[...] = cols
    rows = row_got[0]
    for n in range(1, row_got.shape[0]):
        rows = rows + row_got[n]
    row_left[...] = rows


def finish_kernel(
    sizes, mine, theirs, stored, row_left, weight, row_dual, col_dual, row_out, col_out
):
    _, base, half, _ = sizes
    core = lax.axis_index(CORE)
    step = base * weight[0:1, :]
    row_out[...] = row_dual[...] + step * row_left[...]
    scale = jnp.broadcast_to(step[:, 0:1], (1, half * LANES))
    for side, part in ((core, mine), (1 - core, theirs)):
        lanes = span(side * half, half)
        col_out[:, lanes] = col_dual[:, lanes] + scale * part[...]


VM = pl.BlockSpec(memory_space=pltpu.VMEM)
HB = pl.BlockSpec(memory_space=pltpu.HBM)
ROOM = pltpu.CompilerParams(vmem_limit_bytes=16 << 20)


def shards(cost, plan, row_mass, col_mass, row_dual, col_dual):
    rows, cols = plan.shape
    tiles = cols // LANES
    half = tiles // 2
    narrow = lax.axis_size("narrow")
    wide = lax.axis_size(WIDE)
    chips = wide // 2
    base = 0.9 / math.sqrt(rows * wide + cols * narrow)
    sizes = (narrow, base, half, chips)
    row_mass, row_dual = row_mass.reshape(1, rows), row_dual.reshape(1, rows)
    col_mass, col_dual = col_mass.reshape(1, cols), col_dual.reshape(1, cols)

    def vm(*shape):
        return pltpu.VMEM(shape, jnp.float32)

    def near(*arrays):
        return [pltpu.with_memory_space_constraint(array, pltpu.VMEM) for array in arrays]

    big, state, one, many = vm(rows, cols), vm(GROUP, LANES), vm(1, rows), vm(1, cols)
    give, keep = vm(1, half * LANES), vm(1, (half + 2) * LANES)
    spread = vm(rows, LANES)

    work = pl.CostEstimate(flops=6 * rows * cols, bytes_accessed=0, transcendentals=0)
    sums = vm(MOVED, GROUP, LANES)

    def keep_step(last, *operands):
        share = (one,) if last else ()
        return pl.pallas_call(
            functools.partial(keep_kernel, sizes),
            out_shape=(big, keep) + share,
            in_specs=[VM] * 10,
            out_specs=(VM,) * (2 + len(share)),
            input_output_aliases={3: 0},
            compiler_params=ROOM,
            cost_estimate=work,
            name="keep_step",
        )(*near(*operands))

    inputs = (cost, plan, row_mass, col_mass, row_dual, col_dual)
    outputs = pl.pallas_call(
        functools.partial(open_kernel, sizes),
        out_shape=(big, big, one, many, one, many, big, give, spread, sums, spread, state),
        in_specs=[HB] * 6,
        out_specs=(VM,) * 12,
        scratch_shapes=[pltpu.SemaphoreType.DMA((6, CHUNKS + 1))],
        compiler_params=ROOM,
        cost_estimate=work,
        name="open_step",
    )(*(pltpu.with_memory_space_constraint(array, pltpu.HBM) for array in inputs))
    cost, plan, row_mass, col_mass, row_dual, col_dual = outputs[:6]
    half_plan, given, row_sums, moved_sums, row_all, weight = outputs[6:]
    plan, kept = keep_step(
        False, weight, cost, plan, half_plan, row_mass, col_mass, row_all, col_dual, row_sums,
        moved_sums,
    )
    for step in range(1, ITERS):
        came = swap(given)
        sent = pl.pallas_call(
            functools.partial(build_kernel, sizes),
            out_shape=vm(chips, 1, (half + 2) * LANES),
            in_specs=[VM] * 2,
            out_specs=VM,
            compiler_params=ROOM,
            name="build_step",
        )(*near(kept, came))
        got = exchange(sent, PLANE)
        sent = pl.pallas_call(
            functools.partial(reduce_kernel, sizes),
            out_shape=vm(2 * narrow, 1, (half + chips + 2) * LANES),
            in_specs=[VM],
            out_specs=VM,
            compiler_params=ROOM,
            name="reduce_step",
        )(*near(got))
        got = exchange(sent, COLUMN)
        half_plan, given, row_sums, moved_sums, row_all, weight, row_dual, col_dual = pl.pallas_call(
            functools.partial(give_kernel, sizes),
            out_shape=(big, give, spread, sums, spread, state, one, many),
            in_specs=[VM] * 7,
            out_specs=(VM,) * 8,
            scratch_shapes=[vm(2, 1, chips * LANES)],
            compiler_params=ROOM,
            cost_estimate=work,
            name="give_step",
        )(*near(got, weight, cost, plan, col_mass, row_dual, col_dual))
        plan, kept, *row_sent = keep_step(
            step == ITERS - 1, weight, cost, plan, half_plan, row_mass, col_mass, row_all,
            col_dual, row_sums, moved_sums,
        )
    came = swap(given)
    sent = pl.pallas_call(
        functools.partial(last_build_kernel, sizes),
        out_shape=vm(chips, 1, half * LANES),
        in_specs=[VM] * 2,
        out_specs=VM,
        compiler_params=ROOM,
        name="last_build_step",
    )(*near(kept, came))
    got = exchange(sent, PLANE)
    row_got = lax.all_gather(row_sent[0], "narrow")
    mine, row_left = pl.pallas_call(
        functools.partial(last_reduce_kernel, sizes),
        out_shape=(give, one),
        in_specs=[VM] * 2,
        out_specs=(VM, VM),
        compiler_params=ROOM,
        name="last_reduce_step",
    )(*near(got, row_got))
    theirs = swap(mine)
    plan, stored = pl.pallas_call(
        store_kernel,
        out_shape=(jax.ShapeDtypeStruct((rows, cols), jnp.float32), one),
        in_specs=[VM] * 2,
        out_specs=(HB, VM),
        scratch_shapes=[pltpu.SemaphoreType.DMA],
        compiler_params=ROOM,
        cost_estimate=work,
        name="store_step",
    )(*near(plan, mine))
    row_dual, col_dual = pl.pallas_call(
        functools.partial(finish_kernel, sizes),
        out_shape=tuple(jax.ShapeDtypeStruct(s.shape, s.dtype) for s in (one, many)),
        in_specs=[VM] * 7,
        out_specs=(VM, VM),
        compiler_params=ROOM,
        name="finish_step",
    )(*near(mine, theirs, stored, row_left, weight, row_dual, col_dual))
    return (plan, row_dual.reshape(rows), col_dual.reshape(cols))


def solution(mesh):
    split = Mesh(
        mesh.devices.reshape(4, 4, 2, mesh.shape["narrow"]),
        ("wide_0", "wide_1", "wide_2", "narrow"),
    )
    placed = (P(WIDE, "narrow"), P(WIDE, "narrow"), P(WIDE), P("narrow"), P(WIDE), P("narrow"))
    return jax.shard_map(
        shards,
        mesh=split,
        in_specs=placed,
        out_specs=(P(WIDE, "narrow"), P(WIDE), P("narrow")),
        check_vma=False,
    )
```

```python
import functools
import math

import jax
import jax.numpy as jnp
from jax import lax
from jax.experimental import pallas as pl
from jax.experimental.pallas import tpu as pltpu
from jax.sharding import Mesh
from jax.sharding import PartitionSpec as P


ITERS = 4
LANES = 128
GROUP = 8
CHUNKS = 2
WIDTH = 2
MOVED = 2
CORE = "wide_2"
WIDE = ("wide_0", "wide_1", "wide_2")
COLUMN = ("wide_2", "narrow")
PLANE = ("wide_0", "wide_1")


def exchange(array, axes):
    return lax.all_to_all(array, axes, split_axis=0, concat_axis=0, tiled=True)


def swap(array):
    return lax.ppermute(array, CORE, [(0, 1), (1, 0)])


def total(block):
    return jnp.sum(jnp.sum(block, axis=0, keepdims=True), axis=1, keepdims=True)


def down(block):
    return jnp.sum(block, axis=0, keepdims=True)


def span(start, size):
    return pl.ds(pl.multiple_of(start * LANES, LANES), size * LANES)


def tile_of(n, size=1):
    return slice(n * LANES, (n + size) * LANES)


def collect_kernel(sizes, got, weight, row_dual, new_weight, new_row, row_all, rows_held):
    narrow, base, _, chips = sizes
    core = lax.axis_index(CORE)
    place = lax.axis_index("wide_0") * lax.axis_size("wide_1") + lax.axis_index("wide_1")
    squares, rest = None, None
    for c in range(2):
        part = got[c * narrow]
        for n in range(c * narrow + 1, (c + 1) * narrow):
            part = part + got[n]
        rows, other = part[:, tile_of(0, chips)], part[:, tile_of(chips, 2)]
        rows_held[c] = rows
        squares = rows * rows if squares is None else squares + rows * rows
        rest = other if rest is None else rest + other
    lanes = rest[:, tile_of(0)]
    for p in range(chips):
        lanes = lanes + squares[:, tile_of(p)]
    left_square, moved = total(lanes), total(rest[:, tile_of(1)])
    old = weight[...]
    dual_step = base * old
    dual_moved = dual_step * dual_step * left_square
    new_weight[...] = jnp.sqrt(old * jnp.sqrt((dual_moved + 1.0) / (moved + 1.0)))
    row = row_dual[...] + dual_step[0:1, :] * rows_held[core, :, span(place, 1)]
    new_row[...] = row
    spread_rows(row, row_all)


def col_update(mine, theirs, weight, col_dual, new_col, sizes):
    base, half = sizes[1], sizes[2]
    core = lax.axis_index(CORE)
    scale = jnp.broadcast_to((base * weight[...])[0:1, 0:1], (1, half * LANES))
    for side, part in ((core, mine), (1 - core, theirs)):
        lanes = span(side * half, half)
        new_col[:, lanes] = col_dual[:, lanes] + scale * part[...]


def sweep(step, cost, plan, fresh_plan, row_all, col_dual, tiles, state, done):
    first, count = tiles
    groups = len(state[0])

    def some(m, state):
        rows, moved = list(state[0]), list(state[1])
        cols = [[None, None] for _ in range(WIDTH)]
        lanes = [span(first + WIDTH * m + w, 1) for w in range(WIDTH)]
        duals = [jnp.broadcast_to(col_dual[:, lanes[w]], (GROUP, LANES)) for w in range(WIDTH)]
        for g in range(groups):
            part = slice(g * GROUP, (g + 1) * GROUP)
            both = None
            for w in range(WIDTH):
                old = plan[part, lanes[w]]
                gap = cost[part, lanes[w]] - row_all[part, :] - duals[w]
                fresh = jnp.maximum(old - step * gap, 0.0)
                change = fresh - old
                extrap = fresh + change
                fresh_plan[part, lanes[w]] = fresh
                both = extrap if both is None else both + extrap
                sums = cols[w]
                sums[g % 2] = extrap if sums[g % 2] is None else sums[g % 2] + extrap
                at = (g * WIDTH + w) % len(moved)
                moved[at] = moved[at] + change * change
            rows[g] = rows[g] + both
        for w in range(WIDTH):
            done(WIDTH * m + w, first + WIDTH * m + w, down(cols[w][0] + cols[w][1]))
        return tuple(rows), tuple(moved)

    return lax.fori_loop(0, count // WIDTH, some, state)


def spread_rows(row_dual, row_all):
    row_all[...] = jnp.transpose(jnp.broadcast_to(row_dual, (LANES, LANES)))


def gather_rows(rows):
    return down(jnp.transpose(jnp.concatenate(rows, axis=0)))


def zeros(row_all):
    zero = jnp.zeros((GROUP, LANES), jnp.float32)
    return tuple(zero for _ in range(row_all.shape[0] // GROUP)), (zero,) * MOVED


def into(target, col_mass, wide):
    def done(n, j, cols):
        target[:, span(n, 1)] = col_mass[:, span(j, 1)] * (1.0 / wide) - cols

    return done


def tail(keep, row_mass, state, sizes):
    narrow, _, half, _ = sizes
    keep[:, tile_of(half)] = row_mass[...] * (1.0 / narrow) - gather_rows(state[0])
    keep[:, tile_of(half + 1)] = down(sum(state[1][1:], state[1][0]))


def open_kernel(sizes, *refs):
    _, base, half, chips = sizes
    sources, targets = refs[:6], refs[6:12]
    fresh_plan, give, row_sums, moved_sums, row_all, weight, sems = refs[12:]
    cost, plan, _, col_mass, row_dual, col_dual = targets
    core = lax.axis_index(CORE)
    tiles = half // CHUNKS
    weight[...] = jnp.full((GROUP, LANES), base, jnp.float32)
    small = [pltpu.make_async_copy(sources[n], targets[n], sems.at[n, 0]) for n in range(2, 6)]
    for copy in small:
        copy.start()
    big = []
    for k in range(CHUNKS + 1):
        first = (1 - core) * half + k * tiles if k < CHUNKS else core * half
        lanes = span(first, tiles if k < CHUNKS else half)
        for n in range(2):
            copy = pltpu.make_async_copy(
                sources[n].at[:, lanes], targets[n].at[:, lanes], sems.at[n, k]
            )
            copy.start()
            big.append(copy)
    for copy in small:
        copy.wait()
    spread_rows(row_dual[...], row_all)
    state = zeros(row_all)
    put = into(give, col_mass, 2 * chips)
    for k in range(CHUNKS):
        big[2 * k].wait()
        big[2 * k + 1].wait()
        shift = k * tiles
        state = sweep(
            jnp.float32(1.0), cost, plan, fresh_plan, row_all, col_dual,
            ((1 - core) * half + shift, tiles), state,
            lambda n, j, cols, shift=shift: put(n + shift, j, cols),
        )
    hold(state, row_sums, moved_sums)
    for copy in big[2 * CHUNKS :]:
        copy.wait()


def hold(state, row_sums, moved_sums):
    row_sums[...] = jnp.concatenate(state[0], axis=0)
    for n in range(MOVED):
        moved_sums[n] = state[1][n]


def give_kernel(
    sizes, mine, theirs, weight, new_weight, cost, plan, col_mass, row_all, col_dual,
    fresh_plan, give, row_sums, moved_sums, new_col,
):
    _, base, half, chips = sizes
    col_update(mine, theirs, weight, col_dual, new_col, sizes)
    side = 1 - lax.axis_index(CORE)
    state = sweep(
        base / new_weight[...], cost, plan, fresh_plan, row_all, new_col, (side * half, half),
        zeros(row_all), into(give, col_mass, 2 * chips),
    )
    hold(state, row_sums, moved_sums)


def keep_kernel(
    sizes, weight, cost, plan, half_plan, row_mass, col_mass, row_all, col_dual, row_sums,
    moved_sums, fresh_plan, keep, *last,
):
    _, base, half, chips = sizes
    side = lax.axis_index(CORE)
    copy = None
    if last:
        row_share, plan_out, sem = last
        lanes = span((1 - side) * half, half)
        copy = pltpu.make_async_copy(fresh_plan.at[:, lanes], plan_out.at[:, lanes], sem)
        copy.start()
    rows = row_sums[...]
    groups = row_all.shape[0] // GROUP
    state = tuple(rows[g * GROUP : (g + 1) * GROUP] for g in range(groups)), tuple(
        moved_sums[n] for n in range(MOVED)
    )
    state = sweep(
        base / weight[...], cost, plan, fresh_plan, row_all, col_dual, (side * half, half), state,
        into(keep, col_mass, 2 * chips),
    )
    tail(keep, row_mass, state, sizes)
    if last:
        row_share[...] = keep[:, tile_of(half)]
        copy.wait()


def build_kernel(sizes, keep, came, sent):
    half = sizes[2]
    cols = keep[:, tile_of(0, half)] + came[...]
    rest = keep[:, tile_of(half, 2)]
    for p in range(sent.shape[0]):
        sent[p, :, tile_of(0, half)] = cols
        sent[p, :, tile_of(half, 2)] = rest


def reduce_kernel(sizes, got, mine, sent):
    _, _, half, chips = sizes
    cols = got[0]
    for p in range(1, chips):
        cols = cols + got[p]
    moved = cols[:, tile_of(half + 1)]
    cols = cols[:, tile_of(0, half)]
    mine[...] = cols
    cols = cols * cols
    squares = cols[:, tile_of(0)]
    for r in range(1, half):
        squares = squares + cols[:, tile_of(r)]
    for p in range(chips):
        sent[0, :, tile_of(p)] = got[p, :, tile_of(half)]
    sent[0, :, tile_of(chips)] = squares
    sent[0, :, tile_of(chips + 1)] = moved
    everything = sent[0]
    for q in range(1, sent.shape[0]):
        sent[q] = everything


def last_build_kernel(sizes, keep, came, sent):
    cols = keep[:, tile_of(0, sizes[2])] + came[...]
    for p in range(sent.shape[0]):
        sent[p] = cols


def store_kernel(sizes, plan, after, plan_part, plan_out, stored, sem):
    half = sizes[2]
    lanes = span(lax.axis_index(CORE) * half, half)
    copy = pltpu.make_async_copy(plan.at[:, lanes], plan_out.at[:, lanes], sem)
    copy.start()
    stored[...] = after[:, tile_of(0)]
    copy.wait()


def last_reduce_kernel(got, row_got, mine, row_left):
    cols = got[0]
    for p in range(1, got.shape[0]):
        cols = cols + got[p]
    mine[...] = cols
    rows = row_got[0]
    for n in range(1, row_got.shape[0]):
        rows = rows + row_got[n]
    row_left[...] = rows


def finish_kernel(
    sizes, mine, theirs, stored, row_left, weight, row_dual, col_dual, row_out, col_out
):
    row_out[...] = row_dual[...] + sizes[1] * weight[0:1, :] * row_left[...]
    col_update(mine, theirs, weight, col_dual, col_out, sizes)


VM = pl.BlockSpec(memory_space=pltpu.VMEM)
HB = pl.BlockSpec(memory_space=pltpu.HBM)
ROOM = pltpu.CompilerParams(vmem_limit_bytes=16 << 20)


def shards(cost, plan, row_mass, col_mass, row_dual, col_dual):
    rows, cols = plan.shape
    tiles = cols // LANES
    half = tiles // 2
    narrow = lax.axis_size("narrow")
    wide = lax.axis_size(WIDE)
    chips = wide // 2
    base = 0.9 / math.sqrt(rows * wide + cols * narrow)
    sizes = (narrow, base, half, chips)
    row_mass, row_dual = row_mass.reshape(1, rows), row_dual.reshape(1, rows)
    col_mass, col_dual = col_mass.reshape(1, cols), col_dual.reshape(1, cols)

    def vm(*shape):
        return pltpu.VMEM(shape, jnp.float32)

    big, state, one, many = vm(rows, cols), vm(GROUP, LANES), vm(1, rows), vm(1, cols)
    give, keep = vm(1, half * LANES), vm(1, (half + 2) * LANES)
    spread = vm(rows, LANES)

    work = pl.CostEstimate(flops=6 * rows * cols, bytes_accessed=0, transcendentals=0)
    sums = vm(MOVED, GROUP, LANES)

    whole = jax.ShapeDtypeStruct((rows, cols), jnp.float32)

    def call(kernel, out_shape, *operands, **options):
        place = pltpu.VMEM
        single = not isinstance(out_shape, tuple)
        specs = tuple(HB if o is whole else VM for o in ((out_shape,) if single else out_shape))
        held = options.pop("held", ())
        return pl.pallas_call(
            kernel,
            out_shape=out_shape,
            in_specs=[HB if o in held else VM for o in range(len(operands))],
            out_specs=specs[0] if single else specs,
            compiler_params=ROOM,
            **options,
        )(*(
            pltpu.with_memory_space_constraint(o, pltpu.HBM if n in held else place)
            for n, o in enumerate(operands)
        ))

    def keep_step(last, *operands):
        extra = (one, whole) if last else ()
        return call(
            functools.partial(keep_kernel, sizes), (big, keep) + extra, *operands,
            input_output_aliases={3: 0}, cost_estimate=work,
            scratch_shapes=[pltpu.SemaphoreType.DMA] if last else [],
        )

    inputs = (cost, plan, row_mass, col_mass, row_dual, col_dual)
    outputs = pl.pallas_call(
        functools.partial(open_kernel, sizes),
        out_shape=(big, big, one, many, one, many, big, give, spread, sums, spread, state),
        in_specs=[HB] * 6,
        out_specs=(VM,) * 12,
        scratch_shapes=[pltpu.SemaphoreType.DMA((6, CHUNKS + 1))],
        compiler_params=ROOM,
        cost_estimate=work,
        name="open_step",
    )(*(pltpu.with_memory_space_constraint(array, pltpu.HBM) for array in inputs))
    cost, plan, row_mass, col_mass, row_dual, col_dual = outputs[:6]
    half_plan, given, row_sums, moved_sums, row_all, weight = outputs[6:]
    plan, kept = keep_step(
        False, weight, cost, plan, half_plan, row_mass, col_mass, row_all, col_dual, row_sums,
        moved_sums,
    )
    own = functools.partial
    for step in range(1, ITERS):
        came = swap(given)
        sent = call(own(build_kernel, sizes), vm(chips, 1, (half + 2) * LANES), kept, came)
        got = exchange(sent, PLANE)
        mine, sent = call(
            own(reduce_kernel, sizes),
            (give, vm(2 * narrow, 1, (chips + 2) * LANES)), got,
        )
        theirs = swap(mine)
        got = exchange(sent, COLUMN)
        new_weight, row_dual, row_all = call(
            own(collect_kernel, sizes), (state, one, spread),
            got, weight, row_dual, scratch_shapes=[vm(2, 1, chips * LANES)],
        )
        half_plan, given, row_sums, moved_sums, col_dual = call(
            own(give_kernel, sizes), (big, give, spread, sums, many),
            mine, theirs, weight, new_weight, cost, plan, col_mass, row_all, col_dual,
            cost_estimate=work,
        )
        weight = new_weight
        plan, kept, *tail_parts = keep_step(
            step == ITERS - 1, weight, cost, plan, half_plan, row_mass, col_mass, row_all,
            col_dual, row_sums, moved_sums,
        )
    row_sent, plan_part = tail_parts
    came = swap(given)
    sent = call(own(last_build_kernel, sizes), vm(chips, 1, half * LANES), kept, came)
    got = exchange(sent, PLANE)
    row_got = lax.all_gather(row_sent, "narrow")
    mine, row_left = call(last_reduce_kernel, (give, one), got, row_got)
    theirs = swap(mine)
    plan, stored = call(
        own(store_kernel, sizes), (whole, one), plan, mine, plan_part,
        held=(2,), input_output_aliases={2: 0}, scratch_shapes=[pltpu.SemaphoreType.DMA],
        cost_estimate=work,
    )
    row_out, col_out = call(
        own(finish_kernel, sizes),
        tuple(jax.ShapeDtypeStruct(o.shape, o.dtype) for o in (one, many)),
        mine, theirs, stored, row_left, weight, row_dual, col_dual,
    )
    return (plan, row_out.reshape(rows), col_out.reshape(cols))


def solution(mesh):
    split = Mesh(
        mesh.devices.reshape(4, 4, 2, mesh.shape["narrow"]),
        ("wide_0", "wide_1", "wide_2", "narrow"),
    )
    placed = (P(WIDE, "narrow"), P(WIDE, "narrow"), P(WIDE), P("narrow"), P(WIDE), P("narrow"))
    return jax.shard_map(
        shards,
        mesh=split,
        in_specs=placed,
        out_specs=(P(WIDE, "narrow"), P(WIDE), P("narrow")),
        check_vma=False,
    )
```

```python
import functools
import math

import jax
import jax.numpy as jnp
from jax import lax
from jax.experimental import pallas as pl
from jax.experimental.pallas import tpu as pltpu
from jax.sharding import Mesh
from jax.sharding import PartitionSpec as P


ITERS = 4
LANES = 128
GROUP = 8
CHUNKS = 4
WIDTH = 2
MOVED = 2
CORE = "wide_2"
WIDE = ("wide_0", "wide_1", "wide_2")
COLUMN = ("wide_2", "narrow")
PLANE = ("wide_0", "wide_1")


def exchange(array, axes):
    return lax.all_to_all(array, axes, split_axis=0, concat_axis=0, tiled=True)


def swap(array):
    return lax.ppermute(array, CORE, [(0, 1), (1, 0)])


def total(block):
    return jnp.sum(jnp.sum(block, axis=0, keepdims=True), axis=1, keepdims=True)


def down(block):
    return jnp.sum(block, axis=0, keepdims=True)


def span(start, size):
    return pl.ds(pl.multiple_of(start * LANES, LANES), size * LANES)


def tile_of(n, size=1):
    return slice(n * LANES, (n + size) * LANES)


def collect_kernel(sizes, got, weight, row_dual, new_weight, new_row, row_all, rows_held):
    narrow, base, _, chips = sizes
    core = lax.axis_index(CORE)
    place = lax.axis_index("wide_0") * lax.axis_size("wide_1") + lax.axis_index("wide_1")
    squares, rest = None, None
    for c in range(2):
        part = got[c * narrow]
        for n in range(c * narrow + 1, (c + 1) * narrow):
            part = part + got[n]
        rows, other = part[:, tile_of(0, chips)], part[:, tile_of(chips, 2)]
        rows_held[c] = rows
        squares = rows * rows if squares is None else squares + rows * rows
        rest = other if rest is None else rest + other
    lanes = rest[:, tile_of(0)]
    for p in range(chips):
        lanes = lanes + squares[:, tile_of(p)]
    left_square, moved = total(lanes), total(rest[:, tile_of(1)])
    old = weight[...]
    dual_step = base * old
    dual_moved = dual_step * dual_step * left_square
    new_weight[...] = jnp.sqrt(old * jnp.sqrt((dual_moved + 1.0) / (moved + 1.0)))
    row = row_dual[...] + dual_step[0:1, :] * rows_held[core, :, span(place, 1)]
    new_row[...] = row
    spread_rows(row, row_all)


def col_update(mine, theirs, weight, col_dual, new_col, sizes):
    base, half = sizes[1], sizes[2]
    core = lax.axis_index(CORE)
    scale = jnp.broadcast_to((base * weight[...])[0:1, 0:1], (1, half * LANES))
    for side, part in ((core, mine), (1 - core, theirs)):
        lanes = span(side * half, half)
        new_col[:, lanes] = col_dual[:, lanes] + scale * part[...]


def sweep(step, cost, plan, fresh_plan, row_all, col_dual, tiles, state, done):
    first, count = tiles
    groups = len(state[0])

    def some(m, state):
        rows, moved = list(state[0]), list(state[1])
        cols = [[None, None] for _ in range(WIDTH)]
        lanes = [span(first + WIDTH * m + w, 1) for w in range(WIDTH)]
        duals = [jnp.broadcast_to(col_dual[:, lanes[w]], (GROUP, LANES)) for w in range(WIDTH)]
        for g in range(groups):
            part = slice(g * GROUP, (g + 1) * GROUP)
            both = None
            for w in range(WIDTH):
                old = plan[part, lanes[w]]
                gap = cost[part, lanes[w]] - row_all[part, :] - duals[w]
                fresh = jnp.maximum(old - step * gap, 0.0)
                change = fresh - old
                extrap = fresh + change
                fresh_plan[part, lanes[w]] = fresh
                both = extrap if both is None else both + extrap
                sums = cols[w]
                sums[g % 2] = extrap if sums[g % 2] is None else sums[g % 2] + extrap
                at = (g * WIDTH + w) % len(moved)
                moved[at] = moved[at] + change * change
            rows[g] = rows[g] + both
        for w in range(WIDTH):
            done(WIDTH * m + w, first + WIDTH * m + w, down(cols[w][0] + cols[w][1]))
        return tuple(rows), tuple(moved)

    return lax.fori_loop(0, count // WIDTH, some, state)


def spread_rows(row_dual, row_all):
    row_all[...] = jnp.transpose(jnp.broadcast_to(row_dual, (LANES, LANES)))


def gather_rows(rows):
    return down(jnp.transpose(jnp.concatenate(rows, axis=0)))


def zeros(row_all):
    zero = jnp.zeros((GROUP, LANES), jnp.float32)
    return tuple(zero for _ in range(row_all.shape[0] // GROUP)), (zero,) * MOVED


def into(target, col_mass, wide):
    def done(n, j, cols):
        target[:, span(n, 1)] = col_mass[:, span(j, 1)] * (1.0 / wide) - cols

    return done


def tail(keep, row_mass, state, sizes):
    narrow, _, half, _ = sizes
    keep[:, tile_of(half)] = row_mass[...] * (1.0 / narrow) - gather_rows(state[0])
    keep[:, tile_of(half + 1)] = down(sum(state[1][1:], state[1][0]))


def open_kernel(sizes, *refs):
    _, base, half, chips = sizes
    sources, targets = refs[:6], refs[6:12]
    fresh_plan, give, row_sums, moved_sums, row_all, weight, sems = refs[12:]
    cost, plan, _, col_mass, row_dual, col_dual = targets
    core = lax.axis_index(CORE)
    tiles = half // CHUNKS
    weight[...] = jnp.full((GROUP, LANES), base, jnp.float32)
    small = [pltpu.make_async_copy(sources[n], targets[n], sems.at[n, 0]) for n in range(2, 6)]
    for copy in small:
        copy.start()
    big = []
    for k in range(CHUNKS + 1):
        first = (1 - core) * half + k * tiles if k < CHUNKS else core * half
        lanes = span(first, tiles if k < CHUNKS else half)
        for n in range(2):
            copy = pltpu.make_async_copy(
                sources[n].at[:, lanes], targets[n].at[:, lanes], sems.at[n, k]
            )
            if k < CHUNKS:
                copy.start()
            big.append(copy)
    for copy in small:
        copy.wait()
    spread_rows(row_dual[...], row_all)
    state = zeros(row_all)
    put = into(give, col_mass, 2 * chips)
    for k in range(CHUNKS):
        big[2 * k].wait()
        big[2 * k + 1].wait()
        if k == 0:
            for copy in big[2 * CHUNKS :]:
                copy.start()
        shift = k * tiles
        state = sweep(
            jnp.float32(1.0), cost, plan, fresh_plan, row_all, col_dual,
            ((1 - core) * half + shift, tiles), state,
            lambda n, j, cols, shift=shift: put(n + shift, j, cols),
        )
    hold(state, row_sums, moved_sums)
    for copy in big[2 * CHUNKS :]:
        copy.wait()


def hold(state, row_sums, moved_sums):
    row_sums[...] = jnp.concatenate(state[0], axis=0)
    for n in range(MOVED):
        moved_sums[n] = state[1][n]


def give_kernel(
    sizes, mine, theirs, weight, new_weight, cost, plan, col_mass, row_all, col_dual,
    fresh_plan, give, row_sums, moved_sums, new_col,
):
    _, base, half, chips = sizes
    col_update(mine, theirs, weight, col_dual, new_col, sizes)
    side = 1 - lax.axis_index(CORE)
    state = sweep(
        base / new_weight[...], cost, plan, fresh_plan, row_all, new_col, (side * half, half),
        zeros(row_all), into(give, col_mass, 2 * chips),
    )
    hold(state, row_sums, moved_sums)


def keep_kernel(
    sizes, weight, cost, plan, half_plan, row_mass, col_mass, row_all, col_dual, row_sums,
    moved_sums, fresh_plan, keep, *last,
):
    _, base, half, chips = sizes
    side = lax.axis_index(CORE)
    copy = None
    if last:
        row_share, plan_out, sem = last
        lanes = span((1 - side) * half, half)
        copy = pltpu.make_async_copy(fresh_plan.at[:, lanes], plan_out.at[:, lanes], sem)
        copy.start()
    rows = row_sums[...]
    groups = row_all.shape[0] // GROUP
    state = tuple(rows[g * GROUP : (g + 1) * GROUP] for g in range(groups)), tuple(
        moved_sums[n] for n in range(MOVED)
    )
    state = sweep(
        base / weight[...], cost, plan, fresh_plan, row_all, col_dual, (side * half, half), state,
        into(keep, col_mass, 2 * chips),
    )
    tail(keep, row_mass, state, sizes)
    if last:
        row_share[...] = keep[:, tile_of(half)]
        copy.wait()


def build_kernel(sizes, keep, came, sent):
    half = sizes[2]
    cols = keep[:, tile_of(0, half)] + came[...]
    rest = keep[:, tile_of(half, 2)]
    for p in range(sent.shape[0]):
        sent[p, :, tile_of(0, half)] = cols
        sent[p, :, tile_of(half, 2)] = rest


def reduce_kernel(sizes, got, mine, sent):
    _, _, half, chips = sizes
    cols = got[0]
    for p in range(1, chips):
        cols = cols + got[p]
    moved = cols[:, tile_of(half + 1)]
    cols = cols[:, tile_of(0, half)]
    mine[...] = cols
    cols = cols * cols
    squares = cols[:, tile_of(0)]
    for r in range(1, half):
        squares = squares + cols[:, tile_of(r)]
    for p in range(chips):
        sent[0, :, tile_of(p)] = got[p, :, tile_of(half)]
    sent[0, :, tile_of(chips)] = squares
    sent[0, :, tile_of(chips + 1)] = moved
    everything = sent[0]
    for q in range(1, sent.shape[0]):
        sent[q] = everything


def last_build_kernel(sizes, keep, came, sent):
    cols = keep[:, tile_of(0, sizes[2])] + came[...]
    for p in range(sent.shape[0]):
        sent[p] = cols


def store_kernel(sizes, plan, after, plan_part, plan_out, stored, sem):
    half = sizes[2]
    lanes = span(lax.axis_index(CORE) * half, half)
    copy = pltpu.make_async_copy(plan.at[:, lanes], plan_out.at[:, lanes], sem)
    copy.start()
    stored[...] = after[:, tile_of(0)]
    copy.wait()


def row_kernel(*refs):
    rows = refs[0][...]
    for ref in refs[1:-1]:
        rows = rows + ref[...]
    refs[-1][...] = rows


def last_reduce_kernel(got, mine):
    cols = got[0]
    for p in range(1, got.shape[0]):
        cols = cols + got[p]
    mine[...] = cols


def finish_kernel(
    sizes, mine, theirs, stored, row_left, weight, row_dual, col_dual, row_out, col_out
):
    row_out[...] = row_dual[...] + sizes[1] * weight[0:1, :] * row_left[...]
    col_update(mine, theirs, weight, col_dual, col_out, sizes)


VM = pl.BlockSpec(memory_space=pltpu.VMEM)
HB = pl.BlockSpec(memory_space=pltpu.HBM)
ROOM = pltpu.CompilerParams(vmem_limit_bytes=16 << 20)


def shards(cost, plan, row_mass, col_mass, row_dual, col_dual):
    rows, cols = plan.shape
    tiles = cols // LANES
    half = tiles // 2
    narrow = lax.axis_size("narrow")
    wide = lax.axis_size(WIDE)
    chips = wide // 2
    base = 0.9 / math.sqrt(rows * wide + cols * narrow)
    sizes = (narrow, base, half, chips)
    row_mass, row_dual = row_mass.reshape(1, rows), row_dual.reshape(1, rows)
    col_mass, col_dual = col_mass.reshape(1, cols), col_dual.reshape(1, cols)

    def vm(*shape):
        return pltpu.VMEM(shape, jnp.float32)

    big, state, one, many = vm(rows, cols), vm(GROUP, LANES), vm(1, rows), vm(1, cols)
    give, keep = vm(1, half * LANES), vm(1, (half + 2) * LANES)
    spread = vm(rows, LANES)

    work = pl.CostEstimate(flops=6 * rows * cols, bytes_accessed=0, transcendentals=0)
    sums = vm(MOVED, GROUP, LANES)

    whole = jax.ShapeDtypeStruct((rows, cols), jnp.float32)

    def call(kernel, out_shape, *operands, **options):
        place = pltpu.VMEM
        single = not isinstance(out_shape, tuple)
        specs = tuple(HB if o is whole else VM for o in ((out_shape,) if single else out_shape))
        held = options.pop("held", ())
        return pl.pallas_call(
            kernel,
            out_shape=out_shape,
            in_specs=[HB if o in held else VM for o in range(len(operands))],
            out_specs=specs[0] if single else specs,
            compiler_params=ROOM,
            **options,
        )(*(
            pltpu.with_memory_space_constraint(o, pltpu.HBM if n in held else place)
            for n, o in enumerate(operands)
        ))

    def keep_step(last, *operands):
        extra = (one, whole) if last else ()
        return call(
            functools.partial(keep_kernel, sizes), (big, keep) + extra, *operands,
            input_output_aliases={3: 0}, cost_estimate=work,
            scratch_shapes=[pltpu.SemaphoreType.DMA] if last else [],
        )

    inputs = (cost, plan, row_mass, col_mass, row_dual, col_dual)
    outputs = pl.pallas_call(
        functools.partial(open_kernel, sizes),
        out_shape=(big, big, one, many, one, many, big, give, spread, sums, spread, state),
        in_specs=[HB] * 6,
        out_specs=(VM,) * 12,
        scratch_shapes=[pltpu.SemaphoreType.DMA((6, CHUNKS + 1))],
        compiler_params=ROOM,
        cost_estimate=work,
        name="open_step",
    )(*(pltpu.with_memory_space_constraint(array, pltpu.HBM) for array in inputs))
    cost, plan, row_mass, col_mass, row_dual, col_dual = outputs[:6]
    half_plan, given, row_sums, moved_sums, row_all, weight = outputs[6:]
    plan, kept = keep_step(
        False, weight, cost, plan, half_plan, row_mass, col_mass, row_all, col_dual, row_sums,
        moved_sums,
    )
    own = functools.partial
    for step in range(1, ITERS):
        came = swap(given)
        sent = call(own(build_kernel, sizes), vm(chips, 1, (half + 2) * LANES), kept, came)
        got = exchange(sent, PLANE)
        mine, sent = call(
            own(reduce_kernel, sizes),
            (give, vm(2 * narrow, 1, (chips + 2) * LANES)), got,
        )
        theirs = swap(mine)
        got = exchange(sent, COLUMN)
        new_weight, row_dual, row_all = call(
            own(collect_kernel, sizes), (state, one, spread),
            got, weight, row_dual, scratch_shapes=[vm(2, 1, chips * LANES)],
        )
        half_plan, given, row_sums, moved_sums, col_dual = call(
            own(give_kernel, sizes), (big, give, spread, sums, many),
            mine, theirs, weight, new_weight, cost, plan, col_mass, row_all, col_dual,
            cost_estimate=work,
        )
        weight = new_weight
        plan, kept, *tail_parts = keep_step(
            step == ITERS - 1, weight, cost, plan, half_plan, row_mass, col_mass, row_all,
            col_dual, row_sums, moved_sums,
        )
    row_sent, plan_part = tail_parts
    came = swap(given)
    sent = call(own(last_build_kernel, sizes), vm(chips, 1, half * LANES), kept, came)
    got = exchange(sent, PLANE)
    row_got = [
        lax.ppermute(row_sent, "narrow", [(n, (n + k) % narrow) for n in range(narrow)])
        for k in range(1, narrow)
    ]
    row_left = call(row_kernel, one, row_sent, *row_got)
    mine = call(last_reduce_kernel, give, got)
    theirs = swap(mine)
    plan, stored = call(
        own(store_kernel, sizes), (whole, one), plan, mine, plan_part,
        held=(2,), input_output_aliases={2: 0}, scratch_shapes=[pltpu.SemaphoreType.DMA],
        cost_estimate=work,
    )
    row_out, col_out = call(
        own(finish_kernel, sizes),
        tuple(jax.ShapeDtypeStruct(o.shape, o.dtype) for o in (one, many)),
        mine, theirs, stored, row_left, weight, row_dual, col_dual,
    )
    return (plan, row_out.reshape(rows), col_out.reshape(cols))


def solution(mesh):
    split = Mesh(
        mesh.devices.reshape(4, 4, 2, mesh.shape["narrow"]),
        ("wide_0", "wide_1", "wide_2", "narrow"),
    )
    placed = (P(WIDE, "narrow"), P(WIDE, "narrow"), P(WIDE), P("narrow"), P(WIDE), P("narrow"))
    return jax.shard_map(
        shards,
        mesh=split,
        in_specs=placed,
        out_specs=(P(WIDE, "narrow"), P(WIDE), P("narrow")),
        check_vma=False,
    )
```

```python
import functools
import math

import jax
import jax.numpy as jnp
from jax import lax
from jax.experimental import pallas as pl
from jax.experimental.pallas import tpu as pltpu
from jax.sharding import Mesh
from jax.sharding import PartitionSpec as P


ITERS = 4
LANES = 128
GROUP = 8
CHUNKS = 2
WIDTH = 2
MOVED = 2
CORE = "wide_2"
WIDE = ("wide_0", "wide_1", "wide_2")
COLUMN = ("wide_2", "narrow")


def exchange(array, axes, groups=None):
    return lax.all_to_all(
        array, axes, split_axis=0, concat_axis=0, tiled=True, axis_index_groups=groups
    )


def crossed():
    sizes = [lax.axis_size(axis) for axis in WIDE]
    groups = []
    for side in range(sizes[2]):
        groups.append([
            (a * sizes[1] + b) * sizes[2] + (side ^ (a * 2 // sizes[0]))
            for a in range(sizes[0])
            for b in range(sizes[1])
        ])
    return groups


def own_side():
    upper = (lax.axis_index("wide_0") * 2) // lax.axis_size("wide_0")
    return (lax.axis_index(CORE) + upper) % 2


def swap(array):
    return lax.ppermute(array, CORE, [(0, 1), (1, 0)])


def total(block):
    return jnp.sum(jnp.sum(block, axis=0, keepdims=True), axis=1, keepdims=True)


def down(block):
    return jnp.sum(block, axis=0, keepdims=True)


def span(start, size):
    return pl.ds(pl.multiple_of(start * LANES, LANES), size * LANES)


def tile_of(n, size=1):
    return slice(n * LANES, (n + size) * LANES)


def collect_kernel(sizes, got, weight, row_dual, new_weight, new_row, row_all, rows_held):
    narrow, base, _, chips = sizes
    core = lax.axis_index(CORE)
    place = lax.axis_index("wide_0") * lax.axis_size("wide_1") + lax.axis_index("wide_1")
    squares, rest = None, None
    for c in range(2):
        part = got[c * narrow]
        for n in range(c * narrow + 1, (c + 1) * narrow):
            part = part + got[n]
        rows, other = part[:, tile_of(0, chips)], part[:, tile_of(chips, 2)]
        rows_held[c] = rows
        squares = rows * rows if squares is None else squares + rows * rows
        rest = other if rest is None else rest + other
    lanes = rest[:, tile_of(0)]
    for p in range(chips):
        lanes = lanes + squares[:, tile_of(p)]
    left_square, moved = total(lanes), total(rest[:, tile_of(1)])
    old = weight[...]
    dual_step = base * old
    dual_moved = dual_step * dual_step * left_square
    new_weight[...] = jnp.sqrt(old * jnp.sqrt((dual_moved + 1.0) / (moved + 1.0)))
    row = row_dual[...] + dual_step[0:1, :] * rows_held[core, :, span(place, 1)]
    new_row[...] = row
    spread_rows(row, row_all)


def col_update(mine, theirs, weight, col_dual, new_col, sizes):
    base, half = sizes[1], sizes[2]
    own = own_side()
    scale = jnp.broadcast_to((base * weight[...])[0:1, 0:1], (1, half * LANES))
    for side, part in ((own, mine), (1 - own, theirs)):
        lanes = span(side * half, half)
        new_col[:, lanes] = col_dual[:, lanes] + scale * part[...]


def sweep(step, cost, plan, fresh_plan, row_all, col_dual, tiles, state, done):
    first, count = tiles
    groups = len(state[0])

    def some(m, state):
        rows, moved = list(state[0]), list(state[1])
        cols = [[None, None] for _ in range(WIDTH)]
        lanes = [span(first + WIDTH * m + w, 1) for w in range(WIDTH)]
        duals = [jnp.broadcast_to(col_dual[:, lanes[w]], (GROUP, LANES)) for w in range(WIDTH)]
        for g in range(groups):
            part = slice(g * GROUP, (g + 1) * GROUP)
            both = None
            for w in range(WIDTH):
                old = plan[part, lanes[w]]
                gap = cost[part, lanes[w]] - row_all[part, :] - duals[w]
                fresh = jnp.maximum(old - step * gap, 0.0)
                change = fresh - old
                extrap = fresh + change
                fresh_plan[part, lanes[w]] = fresh
                both = extrap if both is None else both + extrap
                sums = cols[w]
                sums[g % 2] = extrap if sums[g % 2] is None else sums[g % 2] + extrap
                at = (g * WIDTH + w) % len(moved)
                moved[at] = moved[at] + change * change
            rows[g] = rows[g] + both
        for w in range(WIDTH):
            done(WIDTH * m + w, first + WIDTH * m + w, down(cols[w][0] + cols[w][1]))
        return tuple(rows), tuple(moved)

    return lax.fori_loop(0, count // WIDTH, some, state)


def spread_rows(row_dual, row_all):
    row_all[...] = jnp.transpose(jnp.broadcast_to(row_dual, (LANES, LANES)))


def gather_rows(rows):
    return down(jnp.transpose(jnp.concatenate(rows, axis=0)))


def zeros(row_all):
    zero = jnp.zeros((GROUP, LANES), jnp.float32)
    return tuple(zero for _ in range(row_all.shape[0] // GROUP)), (zero,) * MOVED


def into(target, col_mass, wide):
    def done(n, j, cols):
        target[:, span(n, 1)] = col_mass[:, span(j, 1)] * (1.0 / wide) - cols

    return done


def tail(keep, row_mass, state, sizes):
    narrow, _, half, _ = sizes
    keep[:, tile_of(half)] = row_mass[...] * (1.0 / narrow) - gather_rows(state[0])
    keep[:, tile_of(half + 1)] = down(sum(state[1][1:], state[1][0]))


def open_kernel(sizes, *refs):
    _, base, half, chips = sizes
    sources, targets = refs[:6], refs[6:12]
    fresh_plan, give, row_sums, moved_sums, row_all, weight, sems = refs[12:]
    cost, plan, _, col_mass, row_dual, col_dual = targets
    own = own_side()
    tiles = half // CHUNKS
    weight[...] = jnp.full((GROUP, LANES), base, jnp.float32)
    small = [pltpu.make_async_copy(sources[n], targets[n], sems.at[n, 0]) for n in range(2, 6)]
    for copy in small:
        copy.start()
    big = []
    for k in range(CHUNKS + 1):
        first = (1 - own) * half + k * tiles if k < CHUNKS else own * half
        lanes = span(first, tiles if k < CHUNKS else half)
        for n in range(2):
            copy = pltpu.make_async_copy(
                sources[n].at[:, lanes], targets[n].at[:, lanes], sems.at[n, k]
            )
            copy.start()
            big.append(copy)
    for copy in small:
        copy.wait()
    spread_rows(row_dual[...], row_all)
    state = zeros(row_all)
    put = into(give, col_mass, 2 * chips)
    for k in range(CHUNKS):
        big[2 * k].wait()
        big[2 * k + 1].wait()
        shift = k * tiles
        state = sweep(
            jnp.float32(1.0), cost, plan, fresh_plan, row_all, col_dual,
            ((1 - own) * half + shift, tiles), state,
            lambda n, j, cols, shift=shift: put(n + shift, j, cols),
        )
    hold(state, row_sums, moved_sums)
    for copy in big[2 * CHUNKS :]:
        copy.wait()


def hold(state, row_sums, moved_sums):
    row_sums[...] = jnp.concatenate(state[0], axis=0)
    for n in range(MOVED):
        moved_sums[n] = state[1][n]


def give_kernel(
    sizes, mine, theirs, weight, new_weight, cost, plan, col_mass, row_all, col_dual,
    fresh_plan, give, row_sums, moved_sums, new_col,
):
    _, base, half, chips = sizes
    col_update(mine, theirs, weight, col_dual, new_col, sizes)
    side = 1 - own_side()
    state = sweep(
        base / new_weight[...], cost, plan, fresh_plan, row_all, new_col, (side * half, half),
        zeros(row_all), into(give, col_mass, 2 * chips),
    )
    hold(state, row_sums, moved_sums)


def keep_kernel(
    sizes, weight, cost, plan, half_plan, row_mass, col_mass, row_all, col_dual, row_sums,
    moved_sums, fresh_plan, keep, *last,
):
    _, base, half, chips = sizes
    side = own_side()
    copy = None
    if last:
        row_share, plan_out, sem = last
        lanes = span((1 - side) * half, half)
        copy = pltpu.make_async_copy(fresh_plan.at[:, lanes], plan_out.at[:, lanes], sem)
        copy.start()
    rows = row_sums[...]
    groups = row_all.shape[0] // GROUP
    state = tuple(rows[g * GROUP : (g + 1) * GROUP] for g in range(groups)), tuple(
        moved_sums[n] for n in range(MOVED)
    )
    state = sweep(
        base / weight[...], cost, plan, fresh_plan, row_all, col_dual, (side * half, half), state,
        into(keep, col_mass, 2 * chips),
    )
    tail(keep, row_mass, state, sizes)
    if last:
        row_share[...] = keep[:, tile_of(half)]
        copy.wait()


def build_kernel(sizes, keep, came, sent):
    half = sizes[2]
    cols = keep[:, tile_of(0, half)] + came[...]
    rest = keep[:, tile_of(half, 2)]
    for p in range(sent.shape[0]):
        sent[p, :, tile_of(0, half)] = cols
        sent[p, :, tile_of(half, 2)] = rest


def reduce_kernel(sizes, got, mine, sent):
    _, _, half, chips = sizes
    cols = got[0]
    for p in range(1, chips):
        cols = cols + got[p]
    moved = cols[:, tile_of(half + 1)]
    cols = cols[:, tile_of(0, half)]
    mine[...] = cols
    cols = cols * cols
    squares = cols[:, tile_of(0)]
    for r in range(1, half):
        squares = squares + cols[:, tile_of(r)]
    for p in range(chips):
        sent[0, :, tile_of(p)] = got[p, :, tile_of(half)]
    sent[0, :, tile_of(chips)] = squares
    sent[0, :, tile_of(chips + 1)] = moved
    everything = sent[0]
    for q in range(1, sent.shape[0]):
        sent[q] = everything


def last_build_kernel(sizes, keep, came, sent):
    cols = keep[:, tile_of(0, sizes[2])] + came[...]
    for p in range(sent.shape[0]):
        sent[p] = cols


def store_kernel(sizes, plan, after, plan_part, plan_out, stored, sem):
    half = sizes[2]
    lanes = span(own_side() * half, half)
    copy = pltpu.make_async_copy(plan.at[:, lanes], plan_out.at[:, lanes], sem)
    copy.start()
    stored[...] = after[:, tile_of(0)]
    copy.wait()


def row_kernel(*refs):
    rows = refs[0][...]
    for ref in refs[1:-1]:
        rows = rows + ref[...]
    refs[-1][...] = rows


def last_reduce_kernel(got, mine):
    cols = got[0]
    for p in range(1, got.shape[0]):
        cols = cols + got[p]
    mine[...] = cols


def finish_kernel(
    sizes, mine, theirs, stored, row_left, weight, row_dual, col_dual, row_out, col_out
):
    row_out[...] = row_dual[...] + sizes[1] * weight[0:1, :] * row_left[...]
    col_update(mine, theirs, weight, col_dual, col_out, sizes)


VM = pl.BlockSpec(memory_space=pltpu.VMEM)
HB = pl.BlockSpec(memory_space=pltpu.HBM)
ROOM = pltpu.CompilerParams(vmem_limit_bytes=16 << 20)


def shards(cost, plan, row_mass, col_mass, row_dual, col_dual):
    rows, cols = plan.shape
    tiles = cols // LANES
    half = tiles // 2
    narrow = lax.axis_size("narrow")
    wide = lax.axis_size(WIDE)
    chips = wide // 2
    base = 0.9 / math.sqrt(rows * wide + cols * narrow)
    sizes = (narrow, base, half, chips)
    row_mass, row_dual = row_mass.reshape(1, rows), row_dual.reshape(1, rows)
    col_mass, col_dual = col_mass.reshape(1, cols), col_dual.reshape(1, cols)

    def vm(*shape):
        return pltpu.VMEM(shape, jnp.float32)

    big, state, one, many = vm(rows, cols), vm(GROUP, LANES), vm(1, rows), vm(1, cols)
    give, keep = vm(1, half * LANES), vm(1, (half + 2) * LANES)
    spread = vm(rows, LANES)

    work = pl.CostEstimate(flops=6 * rows * cols, bytes_accessed=0, transcendentals=0)
    sums = vm(MOVED, GROUP, LANES)

    whole = jax.ShapeDtypeStruct((rows, cols), jnp.float32)

    def call(kernel, out_shape, *operands, **options):
        place = pltpu.VMEM
        single = not isinstance(out_shape, tuple)
        specs = tuple(HB if o is whole else VM for o in ((out_shape,) if single else out_shape))
        held = options.pop("held", ())
        return pl.pallas_call(
            kernel,
            out_shape=out_shape,
            in_specs=[HB if o in held else VM for o in range(len(operands))],
            out_specs=specs[0] if single else specs,
            compiler_params=ROOM,
            **options,
        )(*(
            pltpu.with_memory_space_constraint(o, pltpu.HBM if n in held else place)
            for n, o in enumerate(operands)
        ))

    def keep_step(last, *operands):
        extra = (one, whole) if last else ()
        return call(
            functools.partial(keep_kernel, sizes), (big, keep) + extra, *operands,
            input_output_aliases={3: 0}, cost_estimate=work,
            scratch_shapes=[pltpu.SemaphoreType.DMA] if last else [],
        )

    inputs = (cost, plan, row_mass, col_mass, row_dual, col_dual)
    outputs = pl.pallas_call(
        functools.partial(open_kernel, sizes),
        out_shape=(big, big, one, many, one, many, big, give, spread, sums, spread, state),
        in_specs=[HB] * 6,
        out_specs=(VM,) * 12,
        scratch_shapes=[pltpu.SemaphoreType.DMA((6, CHUNKS + 1))],
        compiler_params=ROOM,
        cost_estimate=work,
        name="open_step",
    )(*(pltpu.with_memory_space_constraint(array, pltpu.HBM) for array in inputs))
    cost, plan, row_mass, col_mass, row_dual, col_dual = outputs[:6]
    half_plan, given, row_sums, moved_sums, row_all, weight = outputs[6:]
    plan, kept = keep_step(
        False, weight, cost, plan, half_plan, row_mass, col_mass, row_all, col_dual, row_sums,
        moved_sums,
    )
    own = functools.partial
    for step in range(1, ITERS):
        came = swap(given)
        sent = call(own(build_kernel, sizes), vm(chips, 1, (half + 2) * LANES), kept, came)
        got = exchange(sent, WIDE, crossed())
        mine, sent = call(
            own(reduce_kernel, sizes),
            (give, vm(2 * narrow, 1, (chips + 2) * LANES)), got,
        )
        theirs = swap(mine)
        got = exchange(sent, COLUMN)
        new_weight, row_dual, row_all = call(
            own(collect_kernel, sizes), (state, one, spread),
            got, weight, row_dual, scratch_shapes=[vm(2, 1, chips * LANES)],
        )
        half_plan, given, row_sums, moved_sums, col_dual = call(
            own(give_kernel, sizes), (big, give, spread, sums, many),
            mine, theirs, weight, new_weight, cost, plan, col_mass, row_all, col_dual,
            cost_estimate=work,
        )
        weight = new_weight
        plan, kept, *tail_parts = keep_step(
            step == ITERS - 1, weight, cost, plan, half_plan, row_mass, col_mass, row_all,
            col_dual, row_sums, moved_sums,
        )
    row_sent, plan_part = tail_parts
    came = swap(given)
    sent = call(own(last_build_kernel, sizes), vm(chips, 1, half * LANES), kept, came)
    got = exchange(sent, WIDE, crossed())
    row_got = [
        lax.ppermute(row_sent, "narrow", [(n, (n + k) % narrow) for n in range(narrow)])
        for k in range(1, narrow)
    ]
    row_left = call(row_kernel, one, row_sent, *row_got)
    mine = call(last_reduce_kernel, give, got)
    theirs = swap(mine)
    plan, stored = call(
        own(store_kernel, sizes), (whole, one), plan, mine, plan_part,
        held=(2,), input_output_aliases={2: 0}, scratch_shapes=[pltpu.SemaphoreType.DMA],
        cost_estimate=work,
    )
    row_out, col_out = call(
        own(finish_kernel, sizes),
        tuple(jax.ShapeDtypeStruct(o.shape, o.dtype) for o in (one, many)),
        mine, theirs, stored, row_left, weight, row_dual, col_dual,
    )
    return (plan, row_out.reshape(rows), col_out.reshape(cols))


def solution(mesh):
    split = Mesh(
        mesh.devices.reshape(4, 4, 2, mesh.shape["narrow"]),
        ("wide_0", "wide_1", "wide_2", "narrow"),
    )
    placed = (P(WIDE, "narrow"), P(WIDE, "narrow"), P(WIDE), P("narrow"), P(WIDE), P("narrow"))
    return jax.shard_map(
        shards,
        mesh=split,
        in_specs=placed,
        out_specs=(P(WIDE, "narrow"), P(WIDE), P("narrow")),
        check_vma=False,
    )
```

```python
import functools
import math

import jax
import jax.numpy as jnp
from jax import lax
from jax.experimental import pallas as pl
from jax.experimental.pallas import tpu as pltpu
from jax.sharding import Mesh
from jax.sharding import PartitionSpec as P


ITERS = 4
LANES = 128
GROUP = 8
CHUNKS = 2
WIDTH = 2
MOVED = 2
CORE = "wide_2"
WIDE = ("wide_0", "wide_1", "wide_2")
COLUMN = ("wide_2", "narrow")


def exchange(array, axes, groups=None):
    return lax.all_to_all(
        array, axes, split_axis=0, concat_axis=0, tiled=True, axis_index_groups=groups
    )


def turned(place, size):
    return (4 * place + size) // (2 * size) % 2


def crossed():
    sizes = [lax.axis_size(axis) for axis in WIDE]
    groups = []
    for side in range(sizes[2]):
        groups.append([
            (a * sizes[1] + b) * sizes[2] + (side ^ turned(b, sizes[1]))
            for a in range(sizes[0])
            for b in range(sizes[1])
        ])
    return groups


def own_side():
    return (lax.axis_index(CORE) + turned(lax.axis_index("wide_1"), lax.axis_size("wide_1"))) % 2


def swap(array):
    return lax.ppermute(array, CORE, [(0, 1), (1, 0)])


def total(block):
    return jnp.sum(jnp.sum(block, axis=0, keepdims=True), axis=1, keepdims=True)


def down(block):
    return jnp.sum(block, axis=0, keepdims=True)


def span(start, size):
    return pl.ds(pl.multiple_of(start * LANES, LANES), size * LANES)


def tile_of(n, size=1):
    return slice(n * LANES, (n + size) * LANES)


def collect_kernel(sizes, got, weight, row_dual, new_weight, new_row, row_all, rows_held):
    narrow, base, _, chips = sizes
    core = lax.axis_index(CORE)
    place = lax.axis_index("wide_0") * lax.axis_size("wide_1") + lax.axis_index("wide_1")
    squares, rest = None, None
    for c in range(2):
        part = got[c * narrow]
        for n in range(c * narrow + 1, (c + 1) * narrow):
            part = part + got[n]
        rows, other = part[:, tile_of(0, chips)], part[:, tile_of(chips, 2)]
        rows_held[c] = rows
        squares = rows * rows if squares is None else squares + rows * rows
        rest = other if rest is None else rest + other
    lanes = rest[:, tile_of(0)]
    for p in range(chips):
        lanes = lanes + squares[:, tile_of(p)]
    left_square, moved = total(lanes), total(rest[:, tile_of(1)])
    old = weight[...]
    dual_step = base * old
    dual_moved = dual_step * dual_step * left_square
    new_weight[...] = jnp.sqrt(old * jnp.sqrt((dual_moved + 1.0) / (moved + 1.0)))
    row = row_dual[...] + dual_step[0:1, :] * rows_held[core, :, span(place, 1)]
    new_row[...] = row
    spread_rows(row, row_all)


def col_update(mine, theirs, weight, col_dual, new_col, sizes):
    base, half = sizes[1], sizes[2]
    own = own_side()
    scale = jnp.broadcast_to((base * weight[...])[0:1, 0:1], (1, half * LANES))
    for side, part in ((own, mine), (1 - own, theirs)):
        lanes = span(side * half, half)
        new_col[:, lanes] = col_dual[:, lanes] + scale * part[...]


def sweep(step, cost, plan, fresh_plan, row_all, col_dual, tiles, state, done):
    first, count = tiles
    groups = row_all.shape[0] // GROUP

    def some(m, state):
        rows, moved = (list(state[0]), list(state[1])) if state else ((), ())
        cols = [[None, None] for _ in range(WIDTH)]
        lanes = [span(first + WIDTH * m + w, 1) for w in range(WIDTH)]
        duals = [jnp.broadcast_to(col_dual[:, lanes[w]], (GROUP, LANES)) for w in range(WIDTH)]
        for g in range(groups):
            part = slice(g * GROUP, (g + 1) * GROUP)
            both = None
            for w in range(WIDTH):
                old = plan[part, lanes[w]]
                gap = cost[part, lanes[w]] - row_all[part, :] - duals[w]
                fresh = jnp.maximum(old - step * gap, 0.0)
                change = fresh - old
                extrap = fresh + change
                fresh_plan[part, lanes[w]] = fresh
                sums = cols[w]
                sums[g % 2] = extrap if sums[g % 2] is None else sums[g % 2] + extrap
                if state:
                    both = extrap if both is None else both + extrap
                    at = (g * WIDTH + w) % len(moved)
                    moved[at] = moved[at] + change * change
            if state:
                rows[g] = rows[g] + both
        for w in range(WIDTH):
            done(WIDTH * m + w, first + WIDTH * m + w, down(cols[w][0] + cols[w][1]))
        return tuple(rows), tuple(moved)

    if state is None:
        lax.fori_loop(0, count // WIDTH, lambda m, _: some(m, None) and 0, 0, unroll=True)
        return None
    return lax.fori_loop(0, count // WIDTH, some, state, unroll=True)


def catch_up(plan, fresh_plan, tiles, state):
    first, count = tiles
    groups = len(state[0])

    def some(m, state):
        rows, moved = list(state[0]), list(state[1])
        lanes = [span(first + WIDTH * m + w, 1) for w in range(WIDTH)]
        for g in range(groups):
            part = slice(g * GROUP, (g + 1) * GROUP)
            both = None
            for w in range(WIDTH):
                fresh = fresh_plan[part, lanes[w]]
                change = fresh - plan[part, lanes[w]]
                extrap = fresh + change
                both = extrap if both is None else both + extrap
                at = (g * WIDTH + w) % len(moved)
                moved[at] = moved[at] + change * change
            rows[g] = rows[g] + both
        return tuple(rows), tuple(moved)

    return lax.fori_loop(0, count // WIDTH, some, state, unroll=True)


def spread_rows(row_dual, row_all):
    row_all[...] = jnp.transpose(jnp.broadcast_to(row_dual, (LANES, LANES)))


def gather_rows(rows):
    return down(jnp.transpose(jnp.concatenate(rows, axis=0)))


def zeros(row_all):
    zero = jnp.zeros((GROUP, LANES), jnp.float32)
    return tuple(zero for _ in range(row_all.shape[0] // GROUP)), (zero,) * MOVED


def into(target, col_mass, wide):
    def done(n, j, cols):
        target[:, span(n, 1)] = col_mass[:, span(j, 1)] * (1.0 / wide) - cols

    return done


def tail(keep, row_mass, state, sizes):
    narrow, _, half, _ = sizes
    keep[:, tile_of(half)] = row_mass[...] * (1.0 / narrow) - gather_rows(state[0])
    keep[:, tile_of(half + 1)] = down(sum(state[1][1:], state[1][0]))


def open_kernel(sizes, *refs):
    _, base, half, chips = sizes
    sources, targets = refs[:6], refs[6:12]
    fresh_plan, give, row_all, weight, sems = refs[12:]
    cost, plan, _, col_mass, row_dual, col_dual = targets
    own = own_side()
    tiles = half // CHUNKS
    weight[...] = jnp.full((GROUP, LANES), base, jnp.float32)
    small = [pltpu.make_async_copy(sources[n], targets[n], sems.at[n, 0]) for n in range(2, 6)]
    for copy in small:
        copy.start()
    big = []
    for k in range(CHUNKS + 1):
        first = (1 - own) * half + k * tiles if k < CHUNKS else own * half
        lanes = span(first, tiles if k < CHUNKS else half)
        for n in range(2):
            copy = pltpu.make_async_copy(
                sources[n].at[:, lanes], targets[n].at[:, lanes], sems.at[n, k]
            )
            copy.start()
            big.append(copy)
    for copy in small:
        copy.wait()
    spread_rows(row_dual[...], row_all)
    put = into(give, col_mass, 2 * chips)
    for k in range(CHUNKS):
        big[2 * k].wait()
        big[2 * k + 1].wait()
        shift = k * tiles
        sweep(
            jnp.float32(1.0), cost, plan, fresh_plan, row_all, col_dual,
            ((1 - own) * half + shift, tiles), None,
            lambda n, j, cols, shift=shift: put(n + shift, j, cols),
        )
    for copy in big[2 * CHUNKS :]:
        copy.wait()


def give_kernel(
    sizes, mine, theirs, weight, new_weight, cost, plan, col_mass, row_all, col_dual,
    fresh_plan, give, new_col,
):
    _, base, half, chips = sizes
    col_update(mine, theirs, weight, col_dual, new_col, sizes)
    side = 1 - own_side()
    sweep(
        base / new_weight[...], cost, plan, fresh_plan, row_all, new_col, (side * half, half),
        None, into(give, col_mass, 2 * chips),
    )


def keep_kernel(
    sizes, weight, cost, plan, half_plan, row_mass, col_mass, row_all, col_dual,
    fresh_plan, keep, *last,
):
    _, base, half, chips = sizes
    side = own_side()
    copy = None
    if last:
        row_share, plan_out, sem = last
        lanes = span((1 - side) * half, half)
        copy = pltpu.make_async_copy(fresh_plan.at[:, lanes], plan_out.at[:, lanes], sem)
        copy.start()
    state = catch_up(plan, fresh_plan, ((1 - side) * half, half), zeros(row_all))
    state = sweep(
        base / weight[...], cost, plan, fresh_plan, row_all, col_dual, (side * half, half), state,
        into(keep, col_mass, 2 * chips),
    )
    tail(keep, row_mass, state, sizes)
    if last:
        row_share[...] = keep[:, tile_of(half)]
        copy.wait()


def build_kernel(sizes, keep, came, sent):
    half = sizes[2]
    cols = keep[:, tile_of(0, half)] + came[...]
    rest = keep[:, tile_of(half, 2)]
    for p in range(sent.shape[0]):
        sent[p, :, tile_of(0, half)] = cols
        sent[p, :, tile_of(half, 2)] = rest


def reduce_kernel(sizes, got, mine, sent):
    _, _, half, chips = sizes
    cols = got[0]
    for p in range(1, chips):
        cols = cols + got[p]
    moved = cols[:, tile_of(half + 1)]
    cols = cols[:, tile_of(0, half)]
    mine[...] = cols
    cols = cols * cols
    squares = cols[:, tile_of(0)]
    for r in range(1, half):
        squares = squares + cols[:, tile_of(r)]
    for p in range(chips):
        sent[0, :, tile_of(p)] = got[p, :, tile_of(half)]
    sent[0, :, tile_of(chips)] = squares
    sent[0, :, tile_of(chips + 1)] = moved
    everything = sent[0]
    for q in range(1, sent.shape[0]):
        sent[q] = everything


def last_build_kernel(sizes, keep, came, sent):
    cols = keep[:, tile_of(0, sizes[2])] + came[...]
    for p in range(sent.shape[0]):
        sent[p] = cols


def store_kernel(sizes, plan, after, plan_part, plan_out, stored, sem):
    half = sizes[2]
    lanes = span(own_side() * half, half)
    copy = pltpu.make_async_copy(plan.at[:, lanes], plan_out.at[:, lanes], sem)
    copy.start()
    stored[...] = after[:, tile_of(0)]
    copy.wait()


def row_kernel(*refs):
    rows = refs[0][...]
    for ref in refs[1:-1]:
        rows = rows + ref[...]
    refs[-1][...] = rows


def last_reduce_kernel(got, mine):
    cols = got[0]
    for p in range(1, got.shape[0]):
        cols = cols + got[p]
    mine[...] = cols


def finish_kernel(
    sizes, mine, theirs, stored, row_left, weight, row_dual, col_dual, row_out, col_out
):
    row_out[...] = row_dual[...] + sizes[1] * weight[0:1, :] * row_left[...]
    col_update(mine, theirs, weight, col_dual, col_out, sizes)


VM = pl.BlockSpec(memory_space=pltpu.VMEM)
HB = pl.BlockSpec(memory_space=pltpu.HBM)
ROOM = pltpu.CompilerParams(vmem_limit_bytes=16 << 20)


def shards(cost, plan, row_mass, col_mass, row_dual, col_dual):
    rows, cols = plan.shape
    tiles = cols // LANES
    half = tiles // 2
    narrow = lax.axis_size("narrow")
    wide = lax.axis_size(WIDE)
    chips = wide // 2
    base = 0.9 / math.sqrt(rows * wide + cols * narrow)
    sizes = (narrow, base, half, chips)
    row_mass, row_dual = row_mass.reshape(1, rows), row_dual.reshape(1, rows)
    col_mass, col_dual = col_mass.reshape(1, cols), col_dual.reshape(1, cols)

    def vm(*shape):
        return pltpu.VMEM(shape, jnp.float32)

    big, state, one, many = vm(rows, cols), vm(GROUP, LANES), vm(1, rows), vm(1, cols)
    give, keep = vm(1, half * LANES), vm(1, (half + 2) * LANES)
    spread = vm(rows, LANES)

    work = pl.CostEstimate(flops=6 * rows * cols, bytes_accessed=0, transcendentals=0)

    whole = jax.ShapeDtypeStruct((rows, cols), jnp.float32)

    def call(kernel, out_shape, *operands, **options):
        place = pltpu.VMEM
        single = not isinstance(out_shape, tuple)
        specs = tuple(HB if o is whole else VM for o in ((out_shape,) if single else out_shape))
        held = options.pop("held", ())
        return pl.pallas_call(
            kernel,
            out_shape=out_shape,
            in_specs=[HB if o in held else VM for o in range(len(operands))],
            out_specs=specs[0] if single else specs,
            compiler_params=ROOM,
            **options,
        )(*(
            pltpu.with_memory_space_constraint(o, pltpu.HBM if n in held else place)
            for n, o in enumerate(operands)
        ))

    def keep_step(last, *operands):
        extra = (one, whole) if last else ()
        return call(
            functools.partial(keep_kernel, sizes), (big, keep) + extra, *operands,
            input_output_aliases={3: 0}, cost_estimate=work,
            scratch_shapes=[pltpu.SemaphoreType.DMA] if last else [],
        )

    inputs = (cost, plan, row_mass, col_mass, row_dual, col_dual)
    outputs = pl.pallas_call(
        functools.partial(open_kernel, sizes),
        out_shape=(big, big, one, many, one, many, big, give, spread, state),
        in_specs=[HB] * 6,
        out_specs=(VM,) * 10,
        scratch_shapes=[pltpu.SemaphoreType.DMA((6, CHUNKS + 1))],
        compiler_params=ROOM,
        cost_estimate=work,
        name="open_step",
    )(*(pltpu.with_memory_space_constraint(array, pltpu.HBM) for array in inputs))
    cost, plan, row_mass, col_mass, row_dual, col_dual = outputs[:6]
    half_plan, given, row_all, weight = outputs[6:]
    plan, kept = keep_step(
        False, weight, cost, plan, half_plan, row_mass, col_mass, row_all, col_dual
    )
    own = functools.partial
    for step in range(1, ITERS):
        came = swap(given)
        sent = call(own(build_kernel, sizes), vm(chips, 1, (half + 2) * LANES), kept, came)
        got = exchange(sent, WIDE, crossed())
        mine, sent = call(
            own(reduce_kernel, sizes),
            (give, vm(2 * narrow, 1, (chips + 2) * LANES)), got,
        )
        theirs = swap(mine)
        got = exchange(sent, COLUMN)
        new_weight, row_dual, row_all = call(
            own(collect_kernel, sizes), (state, one, spread),
            got, weight, row_dual, scratch_shapes=[vm(2, 1, chips * LANES)],
        )
        half_plan, given, col_dual = call(
            own(give_kernel, sizes), (big, give, many),
            mine, theirs, weight, new_weight, cost, plan, col_mass, row_all, col_dual,
            cost_estimate=work,
        )
        weight = new_weight
        plan, kept, *tail_parts = keep_step(
            step == ITERS - 1, weight, cost, plan, half_plan, row_mass, col_mass, row_all,
            col_dual,
        )
    row_sent, plan_part = tail_parts
    came = swap(given)
    sent = call(own(last_build_kernel, sizes), vm(chips, 1, half * LANES), kept, came)
    got = exchange(sent, WIDE, crossed())
    row_got = [
        lax.ppermute(row_sent, "narrow", [(n, (n + k) % narrow) for n in range(narrow)])
        for k in range(1, narrow)
    ]
    row_left = call(row_kernel, one, row_sent, *row_got)
    mine = call(last_reduce_kernel, give, got)
    theirs = swap(mine)
    plan, stored = call(
        own(store_kernel, sizes), (whole, one), plan, mine, plan_part,
        held=(2,), input_output_aliases={2: 0}, scratch_shapes=[pltpu.SemaphoreType.DMA],
        cost_estimate=work,
    )
    row_out, col_out = call(
        own(finish_kernel, sizes),
        tuple(jax.ShapeDtypeStruct(o.shape, o.dtype) for o in (one, many)),
        mine, theirs, stored, row_left, weight, row_dual, col_dual,
    )
    return (plan, row_out.reshape(rows), col_out.reshape(cols))


def solution(mesh):
    split = Mesh(
        mesh.devices.reshape(4, 4, 2, mesh.shape["narrow"]),
        ("wide_0", "wide_1", "wide_2", "narrow"),
    )
    placed = (P(WIDE, "narrow"), P(WIDE, "narrow"), P(WIDE), P("narrow"), P(WIDE), P("narrow"))
    return jax.shard_map(
        shards,
        mesh=split,
        in_specs=placed,
        out_specs=(P(WIDE, "narrow"), P(WIDE), P("narrow")),
        check_vma=False,
    )
```

```python
import functools
import math

import jax
import jax.numpy as jnp
from jax import lax
from jax.experimental import pallas as pl
from jax.experimental.pallas import tpu as pltpu
from jax.sharding import Mesh
from jax.sharding import PartitionSpec as P


ITERS = 4
LANES = 128
GROUP = 8
CHUNKS = 2
WIDTH = 2
MOVED = 2
CORE = "wide_2"
WIDE = ("wide_0", "wide_1", "wide_2")
COLUMN = ("wide_2", "narrow")


def exchange(array, axes, groups=None):
    return lax.all_to_all(
        array, axes, split_axis=0, concat_axis=0, tiled=True, axis_index_groups=groups
    )


def turned(place, size):
    return (4 * place + size) // (2 * size) % 2


def crossed():
    sizes = [lax.axis_size(axis) for axis in WIDE]
    groups = []
    for side in range(sizes[2]):
        groups.append([
            (a * sizes[1] + b) * sizes[2] + (side ^ turned(a, sizes[0]))
            for b in range(sizes[1])
            for a in range(sizes[0])
        ])
    return groups


def own_side():
    return (lax.axis_index(CORE) + turned(lax.axis_index("wide_0"), lax.axis_size("wide_0"))) % 2


def swap(array):
    return lax.ppermute(array, CORE, [(0, 1), (1, 0)])


def total(block):
    return jnp.sum(jnp.sum(block, axis=0, keepdims=True), axis=1, keepdims=True)


def down(block):
    return jnp.sum(block, axis=0, keepdims=True)


def span(start, size):
    return pl.ds(pl.multiple_of(start * LANES, LANES), size * LANES)


def tile_of(n, size=1):
    return slice(n * LANES, (n + size) * LANES)


def collect_kernel(sizes, got, weight, row_dual, new_weight, new_row, row_all, rows_held):
    narrow, base, _, chips = sizes
    core = lax.axis_index(CORE)
    place = lax.axis_index("wide_1") * lax.axis_size("wide_0") + lax.axis_index("wide_0")
    squares, rest = None, None
    for c in range(2):
        part = got[c * narrow]
        for n in range(c * narrow + 1, (c + 1) * narrow):
            part = part + got[n]
        rows, other = part[:, tile_of(0, chips)], part[:, tile_of(chips, 2)]
        rows_held[c] = rows
        squares = rows * rows if squares is None else squares + rows * rows
        rest = other if rest is None else rest + other
    lanes = rest[:, tile_of(0)]
    for p in range(chips):
        lanes = lanes + squares[:, tile_of(p)]
    left_square, moved = total(lanes), total(rest[:, tile_of(1)])
    old = weight[...]
    dual_step = base * old
    dual_moved = dual_step * dual_step * left_square
    new_weight[...] = jnp.sqrt(old * jnp.sqrt((dual_moved + 1.0) / (moved + 1.0)))
    row = row_dual[...] + dual_step[0:1, :] * rows_held[core, :, span(place, 1)]
    new_row[...] = row
    spread_rows(row, row_all)


def col_update(mine, theirs, weight, col_dual, new_col, sizes):
    base, half = sizes[1], sizes[2]
    own = own_side()
    scale = jnp.broadcast_to((base * weight[...])[0:1, 0:1], (1, half * LANES))
    for side, part in ((own, mine), (1 - own, theirs)):
        lanes = span(side * half, half)
        new_col[:, lanes] = col_dual[:, lanes] + scale * part[...]


def sweep(step, cost, plan, fresh_plan, row_all, col_dual, tiles, state, done, unroll=True):
    first, count = tiles
    groups = row_all.shape[0] // GROUP

    def some(m, state):
        rows, moved = (list(state[0]), list(state[1])) if state else ((), ())
        cols = [[None, None] for _ in range(WIDTH)]
        lanes = [span(first + WIDTH * m + w, 1) for w in range(WIDTH)]
        duals = [jnp.broadcast_to(col_dual[:, lanes[w]], (GROUP, LANES)) for w in range(WIDTH)]
        for g in range(groups):
            part = slice(g * GROUP, (g + 1) * GROUP)
            both = None
            for w in range(WIDTH):
                old = plan[part, lanes[w]]
                gap = cost[part, lanes[w]] - row_all[part, :] - duals[w]
                fresh = jnp.maximum(old - step * gap, 0.0)
                change = fresh - old
                extrap = fresh + change
                fresh_plan[part, lanes[w]] = fresh
                sums = cols[w]
                sums[g % 2] = extrap if sums[g % 2] is None else sums[g % 2] + extrap
                if state:
                    both = extrap if both is None else both + extrap
                    at = (g * WIDTH + w) % len(moved)
                    moved[at] = moved[at] + change * change
            if state:
                rows[g] = rows[g] + both
        for w in range(WIDTH):
            done(WIDTH * m + w, first + WIDTH * m + w, down(cols[w][0] + cols[w][1]))
        return tuple(rows), tuple(moved)

    if state is None:
        lax.fori_loop(0, count // WIDTH, lambda m, _: some(m, None) and 0, 0, unroll=unroll)
        return None
    return lax.fori_loop(0, count // WIDTH, some, state, unroll=unroll)


def catch_up(plan, fresh_plan, tiles, state, unroll=True):
    first, count = tiles
    groups = len(state[0])

    def some(m, state):
        rows, moved = list(state[0]), list(state[1])
        lanes = [span(first + WIDTH * m + w, 1) for w in range(WIDTH)]
        for g in range(groups):
            part = slice(g * GROUP, (g + 1) * GROUP)
            both = None
            for w in range(WIDTH):
                fresh = fresh_plan[part, lanes[w]]
                change = fresh - plan[part, lanes[w]]
                extrap = fresh + change
                both = extrap if both is None else both + extrap
                at = (g * WIDTH + w) % len(moved)
                moved[at] = moved[at] + change * change
            rows[g] = rows[g] + both
        return tuple(rows), tuple(moved)

    return lax.fori_loop(0, count // WIDTH, some, state, unroll=unroll)


def spread_rows(row_dual, row_all):
    row_all[...] = jnp.transpose(jnp.broadcast_to(row_dual, (LANES, LANES)))


def gather_rows(rows):
    return down(jnp.transpose(jnp.concatenate(rows, axis=0)))


def zeros(row_all):
    zero = jnp.zeros((GROUP, LANES), jnp.float32)
    return tuple(zero for _ in range(row_all.shape[0] // GROUP)), (zero,) * MOVED


def into(target, col_mass, wide):
    def done(n, j, cols):
        target[:, span(n, 1)] = col_mass[:, span(j, 1)] * (1.0 / wide) - cols

    return done


def tail(keep, row_mass, state, sizes):
    narrow, _, half, _ = sizes
    keep[:, tile_of(half)] = row_mass[...] * (1.0 / narrow) - gather_rows(state[0])
    keep[:, tile_of(half + 1)] = down(sum(state[1][1:], state[1][0]))


def open_kernel(sizes, *refs):
    _, base, half, chips = sizes
    sources, targets = refs[:6], refs[6:12]
    fresh_plan, give, row_all, weight, sems = refs[12:]
    cost, plan, _, col_mass, row_dual, col_dual = targets
    own = own_side()
    tiles = half // CHUNKS
    weight[...] = jnp.full((GROUP, LANES), base, jnp.float32)
    small = [pltpu.make_async_copy(sources[n], targets[n], sems.at[n, 0]) for n in range(2, 6)]
    for copy in small:
        copy.start()
    big = []
    for k in range(CHUNKS + 1):
        first = (1 - own) * half + k * tiles if k < CHUNKS else own * half
        lanes = span(first, tiles if k < CHUNKS else half)
        for n in range(2):
            copy = pltpu.make_async_copy(
                sources[n].at[:, lanes], targets[n].at[:, lanes], sems.at[n, k]
            )
            copy.start()
            big.append(copy)
    for copy in small:
        copy.wait()
    spread_rows(row_dual[...], row_all)
    put = into(give, col_mass, 2 * chips)
    for k in range(CHUNKS):
        big[2 * k].wait()
        big[2 * k + 1].wait()
        shift = k * tiles
        sweep(
            jnp.float32(1.0), cost, plan, fresh_plan, row_all, col_dual,
            ((1 - own) * half + shift, tiles), None,
            lambda n, j, cols, shift=shift: put(n + shift, j, cols),
        )
    for copy in big[2 * CHUNKS :]:
        copy.wait()


def give_kernel(
    sizes, mine, theirs, weight, new_weight, cost, plan, col_mass, row_all, col_dual,
    fresh_plan, give, new_col,
):
    _, base, half, chips = sizes
    col_update(mine, theirs, weight, col_dual, new_col, sizes)
    side = 1 - own_side()
    sweep(
        base / new_weight[...], cost, plan, fresh_plan, row_all, new_col, (side * half, half),
        None, into(give, col_mass, 2 * chips),
    )


def keep_kernel(
    sizes, weight, cost, plan, half_plan, row_mass, col_mass, row_all, col_dual,
    fresh_plan, keep, *last,
):
    _, base, half, chips = sizes
    side = own_side()
    copy = None
    if last:
        row_share, plan_out, sem = last
        lanes = span((1 - side) * half, half)
        copy = pltpu.make_async_copy(fresh_plan.at[:, lanes], plan_out.at[:, lanes], sem)
        copy.start()
    state = catch_up(plan, fresh_plan, ((1 - side) * half, half), zeros(row_all), not last)
    state = sweep(
        base / weight[...], cost, plan, fresh_plan, row_all, col_dual, (side * half, half), state,
        into(keep, col_mass, 2 * chips), not last,
    )
    tail(keep, row_mass, state, sizes)
    if last:
        row_share[...] = keep[:, tile_of(half)]
        copy.wait()


def build_kernel(sizes, keep, came, sent):
    half = sizes[2]
    cols = keep[:, tile_of(0, half)] + came[...]
    rest = keep[:, tile_of(half, 2)]
    for p in range(sent.shape[0]):
        sent[p, :, tile_of(0, half)] = cols
        sent[p, :, tile_of(half, 2)] = rest


def reduce_kernel(sizes, got, mine, sent):
    _, _, half, chips = sizes
    cols = got[0]
    for p in range(1, chips):
        cols = cols + got[p]
    moved = cols[:, tile_of(half + 1)]
    cols = cols[:, tile_of(0, half)]
    mine[...] = cols
    cols = cols * cols
    squares = cols[:, tile_of(0)]
    for r in range(1, half):
        squares = squares + cols[:, tile_of(r)]
    for p in range(chips):
        sent[0, :, tile_of(p)] = got[p, :, tile_of(half)]
    sent[0, :, tile_of(chips)] = squares
    sent[0, :, tile_of(chips + 1)] = moved
    everything = sent[0]
    for q in range(1, sent.shape[0]):
        sent[q] = everything


def last_build_kernel(sizes, keep, came, sent):
    cols = keep[:, tile_of(0, sizes[2])] + came[...]
    for p in range(sent.shape[0]):
        sent[p] = cols


def store_kernel(sizes, plan, after, plan_part, plan_out, stored, sem):
    half = sizes[2]
    lanes = span(own_side() * half, half)
    copy = pltpu.make_async_copy(plan.at[:, lanes], plan_out.at[:, lanes], sem)
    copy.start()
    stored[...] = after[:, tile_of(0)]
    copy.wait()


def row_kernel(*refs):
    rows = refs[0][...]
    for ref in refs[1:-1]:
        rows = rows + ref[...]
    refs[-1][...] = rows


def last_reduce_kernel(got, mine):
    cols = got[0]
    for p in range(1, got.shape[0]):
        cols = cols + got[p]
    mine[...] = cols


def finish_kernel(
    sizes, mine, theirs, stored, row_left, weight, row_dual, col_dual, row_out, col_out
):
    row_out[...] = row_dual[...] + sizes[1] * weight[0:1, :] * row_left[...]
    col_update(mine, theirs, weight, col_dual, col_out, sizes)


VM = pl.BlockSpec(memory_space=pltpu.VMEM)
HB = pl.BlockSpec(memory_space=pltpu.HBM)
ROOM = pltpu.CompilerParams(vmem_limit_bytes=16 << 20)


def shards(cost, plan, row_mass, col_mass, row_dual, col_dual):
    rows, cols = plan.shape
    tiles = cols // LANES
    half = tiles // 2
    narrow = lax.axis_size("narrow")
    wide = lax.axis_size(WIDE)
    chips = wide // 2
    base = 0.9 / math.sqrt(rows * wide + cols * narrow)
    sizes = (narrow, base, half, chips)
    row_mass, row_dual = row_mass.reshape(1, rows), row_dual.reshape(1, rows)
    col_mass, col_dual = col_mass.reshape(1, cols), col_dual.reshape(1, cols)

    def vm(*shape):
        return pltpu.VMEM(shape, jnp.float32)

    big, state, one, many = vm(rows, cols), vm(GROUP, LANES), vm(1, rows), vm(1, cols)
    give, keep = vm(1, half * LANES), vm(1, (half + 2) * LANES)
    spread = vm(rows, LANES)

    work = pl.CostEstimate(flops=6 * rows * cols, bytes_accessed=0, transcendentals=0)

    whole = jax.ShapeDtypeStruct((rows, cols), jnp.float32)

    def call(kernel, out_shape, *operands, **options):
        place = pltpu.VMEM
        single = not isinstance(out_shape, tuple)
        specs = tuple(HB if o is whole else VM for o in ((out_shape,) if single else out_shape))
        held = options.pop("held", ())
        return pl.pallas_call(
            kernel,
            out_shape=out_shape,
            in_specs=[HB if o in held else VM for o in range(len(operands))],
            out_specs=specs[0] if single else specs,
            compiler_params=ROOM,
            **options,
        )(*(
            pltpu.with_memory_space_constraint(o, pltpu.HBM if n in held else place)
            for n, o in enumerate(operands)
        ))

    def keep_step(last, *operands):
        extra = (one, whole) if last else ()
        return call(
            functools.partial(keep_kernel, sizes), (big, keep) + extra, *operands,
            input_output_aliases={3: 0}, cost_estimate=work,
            scratch_shapes=[pltpu.SemaphoreType.DMA] if last else [],
        )

    inputs = (cost, plan, row_mass, col_mass, row_dual, col_dual)
    outputs = pl.pallas_call(
        functools.partial(open_kernel, sizes),
        out_shape=(big, big, one, many, one, many, big, give, spread, state),
        in_specs=[HB] * 6,
        out_specs=(VM,) * 10,
        scratch_shapes=[pltpu.SemaphoreType.DMA((6, CHUNKS + 1))],
        compiler_params=ROOM,
        cost_estimate=work,
        name="open_step",
    )(*(pltpu.with_memory_space_constraint(array, pltpu.HBM) for array in inputs))
    cost, plan, row_mass, col_mass, row_dual, col_dual = outputs[:6]
    half_plan, given, row_all, weight = outputs[6:]
    plan, kept = keep_step(
        False, weight, cost, plan, half_plan, row_mass, col_mass, row_all, col_dual
    )
    own = functools.partial
    for step in range(1, ITERS):
        came = swap(given)
        sent = call(own(build_kernel, sizes), vm(chips, 1, (half + 2) * LANES), kept, came)
        got = exchange(sent, WIDE, crossed())
        mine, sent = call(
            own(reduce_kernel, sizes),
            (give, vm(2 * narrow, 1, (chips + 2) * LANES)), got,
        )
        theirs = swap(mine)
        got = exchange(sent, COLUMN)
        new_weight, row_dual, row_all = call(
            own(collect_kernel, sizes), (state, one, spread),
            got, weight, row_dual, scratch_shapes=[vm(2, 1, chips * LANES)],
        )
        half_plan, given, col_dual = call(
            own(give_kernel, sizes), (big, give, many),
            mine, theirs, weight, new_weight, cost, plan, col_mass, row_all, col_dual,
            cost_estimate=work,
        )
        weight = new_weight
        plan, kept, *tail_parts = keep_step(
            step == ITERS - 1, weight, cost, plan, half_plan, row_mass, col_mass, row_all,
            col_dual,
        )
    row_sent, plan_part = tail_parts
    came = swap(given)
    sent = call(own(last_build_kernel, sizes), vm(chips, 1, half * LANES), kept, came)
    got = exchange(sent, WIDE, crossed())
    row_got = [
        lax.ppermute(row_sent, "narrow", [(n, (n + k) % narrow) for n in range(narrow)])
        for k in range(1, narrow)
    ]
    row_left = call(row_kernel, one, row_sent, *row_got)
    mine = call(last_reduce_kernel, give, got)
    theirs = swap(mine)
    plan, stored = call(
        own(store_kernel, sizes), (whole, one), plan, mine, plan_part,
        held=(2,), input_output_aliases={2: 0}, scratch_shapes=[pltpu.SemaphoreType.DMA],
        cost_estimate=work,
    )
    row_out, col_out = call(
        own(finish_kernel, sizes),
        tuple(jax.ShapeDtypeStruct(o.shape, o.dtype) for o in (one, many)),
        mine, theirs, stored, row_left, weight, row_dual, col_dual,
    )
    return (plan, row_out.reshape(rows), col_out.reshape(cols))


def solution(mesh):
    split = Mesh(
        mesh.devices.reshape(4, 4, 2, mesh.shape["narrow"]),
        ("wide_0", "wide_1", "wide_2", "narrow"),
    )
    placed = (P(WIDE, "narrow"), P(WIDE, "narrow"), P(WIDE), P("narrow"), P(WIDE), P("narrow"))
    return jax.shard_map(
        shards,
        mesh=split,
        in_specs=placed,
        out_specs=(P(WIDE, "narrow"), P(WIDE), P("narrow")),
        check_vma=False,
    )
```

```python
import functools
import math

import jax
import jax.numpy as jnp
from jax import lax
from jax.experimental import pallas as pl
from jax.experimental.pallas import tpu as pltpu
from jax.sharding import Mesh
from jax.sharding import PartitionSpec as P


ITERS = 4
LANES = 128
GROUP = 8
CHUNKS = 1
WIDTH = 1
MOVED = 2
CORE = "wide_2"
WIDE = ("wide_0", "wide_1", "wide_2")
COLUMN = ("wide_2", "narrow")


def exchange(array, axes, groups=None):
    return lax.all_to_all(
        array, axes, split_axis=0, concat_axis=0, tiled=True, axis_index_groups=groups
    )


def turned(place, size):
    return (4 * place + size) // (2 * size) % 2


def interleaved(place, size):
    return 2 * place % size + 2 * place // size


def crossed():
    sizes = [lax.axis_size(axis) for axis in WIDE]
    groups = []
    for side in range(sizes[2]):
        groups.append([
            (a * sizes[1] + b) * sizes[2] + (side ^ turned(a, sizes[0]))
            for b in sorted(range(sizes[1]), key=lambda b: interleaved(b, sizes[1]))
            for a in range(sizes[0])
        ])
    return groups


def own_side():
    return (lax.axis_index(CORE) + turned(lax.axis_index("wide_0"), lax.axis_size("wide_0"))) % 2


def swap(array):
    return lax.ppermute(array, CORE, [(0, 1), (1, 0)])


def total(block):
    return jnp.sum(jnp.sum(block, axis=0, keepdims=True), axis=1, keepdims=True)


def down(block):
    return jnp.sum(block, axis=0, keepdims=True)


def span(start, size):
    return pl.ds(pl.multiple_of(start * LANES, LANES), size * LANES)


def tile_of(n, size=1):
    return slice(n * LANES, (n + size) * LANES)


def collect_kernel(sizes, got, weight, row_dual, new_weight, new_row, row_all, rows_held):
    narrow, base, _, chips = sizes
    core = lax.axis_index(CORE)
    along = interleaved(lax.axis_index("wide_1"), lax.axis_size("wide_1"))
    place = along * lax.axis_size("wide_0") + lax.axis_index("wide_0")
    squares, rest = None, None
    for c in range(2):
        part = got[c * narrow]
        for n in range(c * narrow + 1, (c + 1) * narrow):
            part = part + got[n]
        rows, other = part[:, tile_of(0, chips)], part[:, tile_of(chips, 2)]
        rows_held[c] = rows
        squares = rows * rows if squares is None else squares + rows * rows
        rest = other if rest is None else rest + other
    lanes = rest[:, tile_of(0)]
    for p in range(chips):
        lanes = lanes + squares[:, tile_of(p)]
    left_square, moved = total(lanes), total(rest[:, tile_of(1)])
    old = weight[...]
    dual_step = base * old
    dual_moved = dual_step * dual_step * left_square
    new_weight[...] = jnp.sqrt(old * jnp.sqrt((dual_moved + 1.0) / (moved + 1.0)))
    row = row_dual[...] + dual_step[0:1, :] * rows_held[core, :, span(place, 1)]
    new_row[...] = row
    spread_rows(row, row_all)


def col_update(mine, theirs, weight, col_dual, new_col, sizes):
    base, half = sizes[1], sizes[2]
    own = own_side()
    scale = jnp.broadcast_to((base * weight[...])[0:1, 0:1], (1, half * LANES))
    for side, part in ((own, mine), (1 - own, theirs)):
        lanes = span(side * half, half)
        new_col[:, lanes] = col_dual[:, lanes] + scale * part[...]


def sweep(step, cost, plan, fresh_plan, row_all, col_dual, tiles, state, done, unroll=True):
    first, count = tiles
    groups = row_all.shape[0] // GROUP

    def some(m, state):
        rows, moved = (list(state[0]), list(state[1])) if state else ((), ())
        cols = [[None, None] for _ in range(WIDTH)]
        lanes = [span(first + WIDTH * m + w, 1) for w in range(WIDTH)]
        duals = [jnp.broadcast_to(col_dual[:, lanes[w]], (GROUP, LANES)) for w in range(WIDTH)]
        for g in range(groups):
            part = slice(g * GROUP, (g + 1) * GROUP)
            both = None
            for w in range(WIDTH):
                old = plan[part, lanes[w]]
                gap = cost[part, lanes[w]] - row_all[part, :] - duals[w]
                fresh = jnp.maximum(old - step * gap, 0.0)
                change = fresh - old
                extrap = fresh + change
                fresh_plan[part, lanes[w]] = fresh
                sums = cols[w]
                sums[g % 2] = extrap if sums[g % 2] is None else sums[g % 2] + extrap
                if state:
                    both = extrap if both is None else both + extrap
                    at = (g * WIDTH + w) % len(moved)
                    moved[at] = moved[at] + change * change
            if state:
                rows[g] = rows[g] + both
        for w in range(WIDTH):
            done(WIDTH * m + w, first + WIDTH * m + w, down(cols[w][0] + cols[w][1]))
        return tuple(rows), tuple(moved)

    if state is None:
        lax.fori_loop(0, count // WIDTH, lambda m, _: some(m, None) and 0, 0, unroll=unroll)
        return None
    return lax.fori_loop(0, count // WIDTH, some, state, unroll=unroll)


def catch_up(plan, fresh_plan, tiles, state, unroll=True):
    first, count = tiles
    groups = len(state[0])

    def some(m, state):
        rows, moved = list(state[0]), list(state[1])
        lanes = [span(first + WIDTH * m + w, 1) for w in range(WIDTH)]
        for g in range(groups):
            part = slice(g * GROUP, (g + 1) * GROUP)
            both = None
            for w in range(WIDTH):
                fresh = fresh_plan[part, lanes[w]]
                change = fresh - plan[part, lanes[w]]
                extrap = fresh + change
                both = extrap if both is None else both + extrap
                at = (g * WIDTH + w) % len(moved)
                moved[at] = moved[at] + change * change
            rows[g] = rows[g] + both
        return tuple(rows), tuple(moved)

    return lax.fori_loop(0, count // WIDTH, some, state, unroll=unroll)


def spread_rows(row_dual, row_all):
    row_all[...] = jnp.transpose(jnp.broadcast_to(row_dual, (LANES, LANES)))


def gather_rows(rows):
    return down(jnp.transpose(jnp.concatenate(rows, axis=0)))


def zeros(row_all):
    zero = jnp.zeros((GROUP, LANES), jnp.float32)
    return tuple(zero for _ in range(row_all.shape[0] // GROUP)), (zero,) * MOVED


def into(target, col_mass, wide):
    def done(n, j, cols):
        target[:, span(n, 1)] = col_mass[:, span(j, 1)] * (1.0 / wide) - cols

    return done


def tail(keep, row_mass, state, sizes):
    narrow, _, half, _ = sizes
    keep[:, tile_of(half)] = row_mass[...] * (1.0 / narrow) - gather_rows(state[0])
    keep[:, tile_of(half + 1)] = down(sum(state[1][1:], state[1][0]))


def open_kernel(sizes, *refs):
    _, base, half, chips = sizes
    sources, targets = refs[:6], refs[6:12]
    fresh_plan, give, row_all, weight, sems = refs[12:]
    cost, plan, _, col_mass, row_dual, col_dual = targets
    own = own_side()
    tiles = half // CHUNKS
    weight[...] = jnp.full((GROUP, LANES), base, jnp.float32)
    small = [pltpu.make_async_copy(sources[n], targets[n], sems.at[n, 0]) for n in range(2, 6)]
    for copy in small:
        copy.start()
    big = []
    for k in range(CHUNKS + 1):
        first = (1 - own) * half + k * tiles if k < CHUNKS else own * half
        lanes = span(first, tiles if k < CHUNKS else half)
        for n in range(2):
            copy = pltpu.make_async_copy(
                sources[n].at[:, lanes], targets[n].at[:, lanes], sems.at[n, k]
            )
            copy.start()
            big.append(copy)
    for copy in small:
        copy.wait()
    spread_rows(row_dual[...], row_all)
    put = into(give, col_mass, 2 * chips)
    for k in range(CHUNKS):
        big[2 * k].wait()
        big[2 * k + 1].wait()
        shift = k * tiles
        sweep(
            jnp.float32(1.0), cost, plan, fresh_plan, row_all, col_dual,
            ((1 - own) * half + shift, tiles), None,
            lambda n, j, cols, shift=shift: put(n + shift, j, cols),
        )
    for copy in big[2 * CHUNKS :]:
        copy.wait()


def give_kernel(
    sizes, mine, theirs, weight, new_weight, cost, plan, col_mass, row_all, col_dual,
    fresh_plan, give, new_col,
):
    _, base, half, chips = sizes
    col_update(mine, theirs, weight, col_dual, new_col, sizes)
    side = 1 - own_side()
    sweep(
        base / new_weight[...], cost, plan, fresh_plan, row_all, new_col, (side * half, half),
        None, into(give, col_mass, 2 * chips),
    )


def keep_kernel(
    sizes, weight, cost, plan, half_plan, row_mass, col_mass, row_all, col_dual,
    fresh_plan, keep, *last,
):
    _, base, half, chips = sizes
    side = own_side()
    copy = None
    if last:
        row_share, plan_out, sem = last
        lanes = span((1 - side) * half, half)
        copy = pltpu.make_async_copy(fresh_plan.at[:, lanes], plan_out.at[:, lanes], sem)
        copy.start()
    state = catch_up(plan, fresh_plan, ((1 - side) * half, half), zeros(row_all), not last)
    state = sweep(
        base / weight[...], cost, plan, fresh_plan, row_all, col_dual, (side * half, half), state,
        into(keep, col_mass, 2 * chips), not last,
    )
    tail(keep, row_mass, state, sizes)
    if last:
        row_share[...] = keep[:, tile_of(half)]
        copy.wait()


def build_kernel(sizes, keep, came, sent):
    half = sizes[2]
    cols = keep[:, tile_of(0, half)] + came[...]
    rest = keep[:, tile_of(half, 2)]
    for p in range(sent.shape[0]):
        sent[p, :, tile_of(0, half)] = cols
        sent[p, :, tile_of(half, 2)] = rest


def reduce_kernel(sizes, got, mine, sent):
    _, _, half, chips = sizes
    cols = got[0]
    for p in range(1, chips):
        cols = cols + got[p]
    moved = cols[:, tile_of(half + 1)]
    cols = cols[:, tile_of(0, half)]
    mine[...] = cols
    cols = cols * cols
    squares = cols[:, tile_of(0)]
    for r in range(1, half):
        squares = squares + cols[:, tile_of(r)]
    for p in range(chips):
        sent[0, :, tile_of(p)] = got[p, :, tile_of(half)]
    sent[0, :, tile_of(chips)] = squares
    sent[0, :, tile_of(chips + 1)] = moved
    everything = sent[0]
    for q in range(1, sent.shape[0]):
        sent[q] = everything


def last_build_kernel(sizes, keep, came, sent):
    cols = keep[:, tile_of(0, sizes[2])] + came[...]
    for p in range(sent.shape[0]):
        sent[p] = cols


def store_kernel(sizes, plan, after, plan_part, plan_out, stored, sem):
    half = sizes[2]
    lanes = span(own_side() * half, half)
    copy = pltpu.make_async_copy(plan.at[:, lanes], plan_out.at[:, lanes], sem)
    copy.start()
    stored[...] = after[:, tile_of(0)]
    copy.wait()


def row_kernel(*refs):
    rows = refs[0][...]
    for ref in refs[1:-1]:
        rows = rows + ref[...]
    refs[-1][...] = rows


def last_reduce_kernel(got, mine):
    cols = got[0]
    for p in range(1, got.shape[0]):
        cols = cols + got[p]
    mine[...] = cols


def finish_kernel(
    sizes, mine, theirs, stored, row_left, weight, row_dual, col_dual, row_out, col_out
):
    row_out[...] = row_dual[...] + sizes[1] * weight[0:1, :] * row_left[...]
    col_update(mine, theirs, weight, col_dual, col_out, sizes)


VM = pl.BlockSpec(memory_space=pltpu.VMEM)
HB = pl.BlockSpec(memory_space=pltpu.HBM)
ROOM = pltpu.CompilerParams(vmem_limit_bytes=16 << 20)


def shards(cost, plan, row_mass, col_mass, row_dual, col_dual):
    rows, cols = plan.shape
    tiles = cols // LANES
    half = tiles // 2
    narrow = lax.axis_size("narrow")
    wide = lax.axis_size(WIDE)
    chips = wide // 2
    base = 0.9 / math.sqrt(rows * wide + cols * narrow)
    sizes = (narrow, base, half, chips)
    row_mass, row_dual = row_mass.reshape(1, rows), row_dual.reshape(1, rows)
    col_mass, col_dual = col_mass.reshape(1, cols), col_dual.reshape(1, cols)

    def vm(*shape):
        return pltpu.VMEM(shape, jnp.float32)

    big, state, one, many = vm(rows, cols), vm(GROUP, LANES), vm(1, rows), vm(1, cols)
    give, keep = vm(1, half * LANES), vm(1, (half + 2) * LANES)
    spread = vm(rows, LANES)

    work = pl.CostEstimate(flops=6 * rows * cols, bytes_accessed=0, transcendentals=0)

    whole = jax.ShapeDtypeStruct((rows, cols), jnp.float32)

    def call(kernel, out_shape, *operands, **options):
        place = pltpu.VMEM
        single = not isinstance(out_shape, tuple)
        specs = tuple(HB if o is whole else VM for o in ((out_shape,) if single else out_shape))
        held = options.pop("held", ())
        return pl.pallas_call(
            kernel,
            out_shape=out_shape,
            in_specs=[HB if o in held else VM for o in range(len(operands))],
            out_specs=specs[0] if single else specs,
            compiler_params=ROOM,
            **options,
        )(*(
            pltpu.with_memory_space_constraint(o, pltpu.HBM if n in held else place)
            for n, o in enumerate(operands)
        ))

    def keep_step(last, *operands):
        extra = (one, whole) if last else ()
        return call(
            functools.partial(keep_kernel, sizes), (big, keep) + extra, *operands,
            input_output_aliases={3: 0}, cost_estimate=work,
            scratch_shapes=[pltpu.SemaphoreType.DMA] if last else [],
        )

    inputs = (cost, plan, row_mass, col_mass, row_dual, col_dual)
    outputs = pl.pallas_call(
        functools.partial(open_kernel, sizes),
        out_shape=(big, big, one, many, one, many, big, give, spread, state),
        in_specs=[HB] * 6,
        out_specs=(VM,) * 10,
        scratch_shapes=[pltpu.SemaphoreType.DMA((6, CHUNKS + 1))],
        compiler_params=ROOM,
        cost_estimate=work,
        name="open_step",
    )(*(pltpu.with_memory_space_constraint(array, pltpu.HBM) for array in inputs))
    cost, plan, row_mass, col_mass, row_dual, col_dual = outputs[:6]
    half_plan, given, row_all, weight = outputs[6:]
    plan, kept = keep_step(
        False, weight, cost, plan, half_plan, row_mass, col_mass, row_all, col_dual
    )
    own = functools.partial
    for step in range(1, ITERS):
        came = swap(given)
        sent = call(own(build_kernel, sizes), vm(chips, 1, (half + 2) * LANES), kept, came)
        got = exchange(sent, WIDE, crossed())
        mine, sent = call(
            own(reduce_kernel, sizes),
            (give, vm(2 * narrow, 1, (chips + 2) * LANES)), got,
        )
        theirs = swap(mine)
        got = exchange(sent, COLUMN)
        new_weight, row_dual, row_all = call(
            own(collect_kernel, sizes), (state, one, spread),
            got, weight, row_dual, scratch_shapes=[vm(2, 1, chips * LANES)],
        )
        half_plan, given, col_dual = call(
            own(give_kernel, sizes), (big, give, many),
            mine, theirs, weight, new_weight, cost, plan, col_mass, row_all, col_dual,
            cost_estimate=work,
        )
        weight = new_weight
        plan, kept, *tail_parts = keep_step(
            step == ITERS - 1, weight, cost, plan, half_plan, row_mass, col_mass, row_all,
            col_dual,
        )
    row_sent, plan_part = tail_parts
    came = swap(given)
    sent = call(own(last_build_kernel, sizes), vm(chips, 1, half * LANES), kept, came)
    got = exchange(sent, WIDE, crossed())
    row_got = [
        lax.ppermute(row_sent, "narrow", [(n, (n + k) % narrow) for n in range(narrow)])
        for k in range(1, narrow)
    ]
    row_left = call(row_kernel, one, row_sent, *row_got)
    mine = call(last_reduce_kernel, give, got)
    theirs = swap(mine)
    plan, stored = call(
        own(store_kernel, sizes), (whole, one), plan, mine, plan_part,
        held=(2,), input_output_aliases={2: 0}, scratch_shapes=[pltpu.SemaphoreType.DMA],
        cost_estimate=work,
    )
    row_out, col_out = call(
        own(finish_kernel, sizes),
        tuple(jax.ShapeDtypeStruct(o.shape, o.dtype) for o in (one, many)),
        mine, theirs, stored, row_left, weight, row_dual, col_dual,
    )
    return (plan, row_out.reshape(rows), col_out.reshape(cols))


def solution(mesh):
    split = Mesh(
        mesh.devices.reshape(4, 4, 2, mesh.shape["narrow"]),
        ("wide_0", "wide_1", "wide_2", "narrow"),
    )
    placed = (P(WIDE, "narrow"), P(WIDE, "narrow"), P(WIDE), P("narrow"), P(WIDE), P("narrow"))
    return jax.shard_map(
        shards,
        mesh=split,
        in_specs=placed,
        out_specs=(P(WIDE, "narrow"), P(WIDE), P("narrow")),
        check_vma=False,
    )
```
